256 devices in a mesh: lines: 4 (over y), buses: 64 (over z, x, core).
Axes of the slice: x: 4, y: 4, z: 8, core: 2. Of those that a mesh axis runs over, the one named last changes fastest.
Arguments:
- ptdf: bfloat16 [4096, 81920], P('lines', 'buses'), may hold values from -0.0625 to 0.0625
- load: float32 [384, 81920], P(None, 'buses'), may hold values from 0.03 to 3.8, as said below
- ratings: float32 [32768], replicated, may hold values from 0.3 to 3
- line_index: int32 [4096], P('lines'), may hold values from 0 to 32767
- gen_bus: int32 [16384], P('buses'), may hold values from 0 to 81919, as said below
- gen_quad: float32 [16384], P('buses'), may hold values from 0.05 to 0.5
- gen_lin: float32 [16384], P('buses'), may hold values from 0.5 to 2.5
- gen_max: float32 [16384], P('buses'), may hold values from 0.8 to 4
- gen_start: float32 [384, 16384], P(None, 'buses'), may hold values from 0 to 2
- stor_bus: int32 [8192], P('buses'), may hold values from 0 to 1279
- stor_quad: float32 [8192], P('buses'), may hold values from 0.05 to 0.5
- stor_rate: float32 [8192], P('buses'), may hold values from 0.3 to 1.5
- stor_energy: float32 [8192], P('buses'), may hold values from 1 to 8
- stor_start: float32 [384, 8192], P(None, 'buses'), may hold values from -0.5 to 0.5
- lam_start: float32 [384], replicated, may hold values from -4 to 4
- mu_start: float32 [384, 4096], P(None, ('lines', 'buses')), may hold values from -3 to 3
- omega_start: float32 [384, 8192], P(None, 'buses'), may hold values from -2 to 2
Outputs:
- gen_out: float32 [384, 16384], P(None, 'buses')
- stor_out: float32 [384, 8192], P(None, 'buses')
- lam_out: float32 [384], replicated
- mu_out: float32 [384, 4096], P(None, ('lines', 'buses'))
- omega_out: float32 [384, 8192], P(None, 'buses')
The draws below stay inside these ranges and needn't reach their ends.
Inputs may be any that keep to these rules, and one draw needn't show every extreme that they name: `gen_bus`: of the 256 generators of one area at most 8 sit on the buses of any one area (1280 consecutive buses); in every draw one area holds exactly 8 generators of every area, and the others of an area spread over the remaining areas as evenly as counts allow. `load`: loads are positive.
All inputs are finite; a program needn't handle non-finite values.
Results may differ from the reference program's by a relative error of at most 0.0075.
Values may be sent and summed in bfloat16 or wider, within the bound.
No kernel may reach another device: no remote copies, remote signals or barrier semaphores. Data moves between devices by JAX's collectives and lax.ppermute only.
A program may use at most 64 MiB of HBM per device.

```python
import math
import jax
import jax.numpy as jnp

HOURS = 24
BUS_DEV = 1280
GEN_DEV = 256
STOR_DEV = 128
RATED = 32768
ROWS = 384
BUSES = 81920
LINES = 4096
GENS = 16384
STOR = 8192


def draw_load(key, part):
    area_count = BUSES // BUS_DEV
    bus_key, row_key, cell_key = jax.random.split(jax.random.fold_in(key, 11), 3)
    area_of = (jnp.arange(BUSES, dtype=jnp.int32) // BUS_DEV).astype(jnp.float32)
    rising = 1.0 + 2.0 * area_of / max(area_count - 1, 1)
    bus_factor = jax.random.uniform(bus_key, (BUSES,), jnp.float32, 0.5, 1.5)
    row_factor = jax.random.uniform(row_key, (ROWS, 1), jnp.float32, 0.7, 1.3)
    cell_factor = jax.random.uniform(cell_key, (ROWS, BUSES), jnp.float32, 0.8, 1.2)
    return (0.3 * rising[None, :] * bus_factor[None, :] * row_factor * cell_factor).astype(jnp.float32)


def draw_gen_bus(key, part):
    area_count = GENS // GEN_DEV
    slot_count = max(8, (GEN_DEV + area_count - 1) // area_count)
    hot_key, order_key, other_key, bus_key = jax.random.split(jax.random.fold_in(key, 23), 4)
    hot_area = jax.random.randint(hot_key, (), 0, area_count)
    position = jax.vmap(lambda sub_key: jax.random.permutation(sub_key, GEN_DEV))(jax.random.split(order_key, area_count))
    others = jax.vmap(lambda sub_key: jax.random.permutation(sub_key, area_count - 1))(jax.random.split(other_key, area_count))
    spill_index = jnp.maximum(position - slot_count, 0) % (area_count - 1)
    offset = jnp.take_along_axis(others, spill_index, axis=1)
    target = jnp.where(position < slot_count, hot_area, (hot_area + 1 + offset) % area_count)
    local_bus = jax.random.randint(bus_key, (area_count, GEN_DEV), 0, BUS_DEV)
    return (target * BUS_DEV + local_bus).reshape(GENS).astype(jnp.int32)


def plant(result, own_key, low, top_value):
    longest = result.shape.index(max(result.shape))
    spots = []
    for shift in (0, 1):
        where = [jax.random.randint(jax.random.fold_in(own_key, axis), (), 0, length) for axis, length in enumerate(result.shape)]
        where[longest] = (where[longest] + shift) % result.shape[longest]
        spots.append(tuple(where))
    return result.at[spots[0]].set(low).at[spots[1]].set(top_value)


def with_spikes(result, stream_key, source, target, parts, factor):
    def block_of(dim):
        return (jnp.arange(result.shape[dim]) // (result.shape[dim] // parts)).reshape((-1,) + (1,) * (result.ndim - 1 - dim))

    first = jax.random.permutation(stream_key, parts)[block_of(target)]
    other_side = (block_of(target) + parts // 2) % parts
    return jnp.where((block_of(source) == first) | (block_of(source) == other_side), factor * result, result)


def block_levels(key, shape, cuts, low, largest):
    def one(dim, parts):
        heights = jax.random.uniform(jax.random.fold_in(jax.random.fold_in(key, 6), dim), (parts,), jnp.float32, low / len(cuts), largest / len(cuts))
        return jnp.repeat(jnp.exp(heights), shape[dim] // parts).reshape((-1,) + (1,) * (len(shape) - dim - 1))

    factor_of = one(*cuts[0])
    for cut in cuts[1:]:
        factor_of = factor_of * one(*cut)
    return factor_of


def normal_values(stream_key, dims, deviation, most, shards=(), kind=jnp.bfloat16):
    factor_of = block_levels(stream_key, dims, shards, -0.22, 0.18) if shards else 1.0
    result = jax.random.normal(stream_key, dims, jnp.float32) * deviation * factor_of
    return jnp.minimum(jnp.maximum(result, -most), most).astype(kind)


def bell_draw_with(own_key, dims, spread, reach, cuts, heavy, kind=jnp.bfloat16):
    result = spread * jax.random.normal(own_key, dims, jnp.float32)
    if cuts:
        result = result * block_levels(own_key, dims, cuts, -0.22, 0.18)
    return jnp.clip(with_spikes(result, jax.random.fold_in(own_key, 3), *heavy), -reach, reach).astype(kind)


def setup_inputs(seed: int = 0) -> dict:
    splits = jax.random.split(jax.random.key(seed), 18)
    ptdf = bell_draw_with(splits[0], (LINES, BUSES), BUSES ** -0.5, 0.0625, ((0, 4), (1, 64)), (1, 0, 64, 4.0))
    load = draw_load(jax.random.fold_in(splits[17], 71), 0)
    ratings = jnp.clip(jnp.exp(jax.random.uniform(splits[2], (RATED,), jnp.float32, math.log(0.3), math.log(3.0))), 0.3, 3.0)
    line_index = plant(jax.random.randint(splits[3], (LINES,), 0, RATED), jax.random.fold_in(splits[3], 1), 0, RATED - 1).astype(jnp.int32)
    gen_bus = draw_gen_bus(jax.random.fold_in(splits[17], 71), 0)
    gen_quad = jnp.clip(jnp.exp(math.log(0.5) - 2.3025851 * jax.random.uniform(splits[5], (GENS,), jnp.float32) ** block_levels(splits[5], (GENS,), ((0, 64),), -0.2, 0.2)), 0.05, 0.5)
    gen_lin = jnp.clip(0.5 + 2.0 * jax.random.uniform(splits[6], (GENS,), jnp.float32) ** block_levels(splits[6], (GENS,), ((0, 64),), -0.2, 0.2), 0.5, 2.5)
    gen_max = jnp.clip(jnp.exp(math.log(4.0) - 1.609438 * jax.random.uniform(splits[7], (GENS,), jnp.float32) ** block_levels(splits[7], (GENS,), ((0, 64),), -0.2, 0.2)), 0.8, 4.0)
    gen_start = jnp.clip(2.0 * jax.random.uniform(splits[8], (ROWS, GENS), jnp.float32) ** block_levels(splits[8], (ROWS, GENS), ((1, 64),), -0.2, 0.2), 0.0, 2.0)
    stor_bus = plant(jax.random.randint(splits[9], (STOR,), 0, BUS_DEV), jax.random.fold_in(splits[9], 1), 0, BUS_DEV - 1).astype(jnp.int32)
    stor_quad = jnp.clip(jnp.exp(math.log(0.5) - 2.3025851 * jax.random.uniform(splits[10], (STOR,), jnp.float32) ** block_levels(splits[10], (STOR,), ((0, 64),), -0.2, 0.2)), 0.05, 0.5)
    stor_rate = jnp.clip(jnp.exp(math.log(1.5) - 1.60943787 * jax.random.uniform(splits[11], (STOR,), jnp.float32) ** block_levels(splits[11], (STOR,), ((0, 64),), -0.2, 0.2)), 0.3, 1.5)
    stor_energy = jnp.clip(jnp.exp(math.log(8.0) - 2.0794415 * jax.random.uniform(splits[12], (STOR,), jnp.float32) ** block_levels(splits[12], (STOR,), ((0, 64),), -0.2, 0.2)), 1.0, 8.0)
    stor_start = jnp.clip(jax.random.uniform(splits[13], (ROWS, STOR), jnp.float32, -0.5, 0.5) * block_levels(splits[13], (ROWS, STOR), ((1, 64),), -0.4, 0.0), -0.5, 0.5)
    lam_start = normal_values(splits[14], (ROWS,), 1.0, 4.0, (), jnp.float32)
    mu_start = normal_values(splits[15], (ROWS, LINES), 0.5, 3.0, ((1, 256),), jnp.float32)
    omega_start = normal_values(splits[16], (ROWS, STOR), 0.3, 2.0, ((1, 64),), jnp.float32)
    return dict(ptdf=ptdf, load=load, ratings=ratings, line_index=line_index, gen_bus=gen_bus, gen_quad=gen_quad, gen_lin=gen_lin, gen_max=gen_max, gen_start=gen_start, stor_bus=stor_bus, stor_quad=stor_quad, stor_rate=stor_rate, stor_energy=stor_energy, stor_start=stor_start, lam_start=lam_start, mu_start=mu_start, omega_start=omega_start)


TAU = 0.25
SIGMA_FLOW = 4.0
SIGMA_STORE = 0.25
KAPPA = 1.0
THETA = 0.5


def reverse_cum(values, hour_count):
    total_rows, columns = values.shape
    shaped = values.reshape(total_rows // hour_count, hour_count, columns)
    summed = jnp.flip(jnp.cumsum(jnp.flip(shaped, 1), axis=1), 1)
    return summed.reshape(total_rows, columns)


def forward_cum(values, hour_count):
    total_rows, columns = values.shape
    shaped = values.reshape(total_rows // hour_count, hour_count, columns)
    return jnp.cumsum(shaped, axis=1).reshape(total_rows, columns)


def dual_step(dual_now, image_term, step_size, low_bound, high_bound):
    shifted = dual_now + step_size * image_term
    return shifted - step_size * jnp.clip(shifted / step_size, low_bound, high_bound)


def reference(ptdf, load, ratings, line_index, gen_bus, gen_quad, gen_lin, gen_max, gen_start,
              stor_bus, stor_quad, stor_rate, stor_energy, stor_start, lam_start, mu_start, omega_start):
    stor_global = (jnp.arange(STOR, dtype=jnp.int32) // STOR_DEV) * BUS_DEV + stor_bus.astype(jnp.int32)
    gen_index = gen_bus.astype(jnp.int32)
    limit = jnp.take(ratings, line_index.astype(jnp.int32))
    hour_of = jnp.arange(ROWS, dtype=jnp.int32) % HOURS
    last_hour = (hour_of == HOURS - 1)[:, None]
    half_energy = (0.5 * stor_energy)[None, :]
    low_bound = jnp.where(last_hour, jnp.zeros_like(half_energy), -half_energy)
    high_bound = jnp.where(last_hour, jnp.zeros_like(half_energy), half_energy)
    load_total = jnp.sum(load, axis=1)
    gen_now, stor_now = gen_start, stor_start
    gen_old, stor_old = gen_start, stor_start
    price_level, dual_flow, dual_store = lam_start, mu_start, omega_start
    for iteration in range(2):
        if iteration == 0:
            gen_mid, stor_mid = gen_now, stor_now
        else:
            gen_mid = gen_now + THETA * (gen_now - gen_old)
            stor_mid = stor_now + THETA * (stor_now - stor_old)
        bus_price = jnp.dot(dual_flow.astype(jnp.bfloat16), ptdf, preferred_element_type=jnp.float32)
        gen_price = jnp.take(bus_price, gen_index, axis=1)
        stor_price = jnp.take(bus_price, stor_global, axis=1)
        gen_grad = 2.0 * gen_quad * gen_mid + gen_lin + price_level[:, None] + gen_price
        gen_next = jnp.clip(gen_mid - TAU * gen_grad, 0.0, gen_max)
        stor_grad = 2.0 * stor_quad * stor_mid + price_level[:, None] + stor_price + reverse_cum(dual_store, HOURS)
        stor_next = jnp.clip(stor_mid - TAU * stor_grad, -stor_rate, stor_rate)
        gen_bar = 2.0 * gen_next - gen_now
        stor_bar = 2.0 * stor_next - stor_now
        gen_inject = jax.ops.segment_sum(gen_bar.T, gen_index, num_segments=BUSES).T
        stor_inject = jax.ops.segment_sum(stor_bar.T, stor_global, num_segments=BUSES).T
        injection = gen_inject + stor_inject - load
        flow_sum = jnp.dot(injection.astype(jnp.bfloat16), ptdf.T, preferred_element_type=jnp.float32)
        dual_flow = dual_step(dual_flow, flow_sum, SIGMA_FLOW, -limit, limit)
        balance = jnp.sum(gen_bar, axis=1) + jnp.sum(stor_bar, axis=1) - load_total
        price_level = price_level + (KAPPA / (GENS + STOR)) * balance
        dual_store = dual_step(dual_store, forward_cum(stor_bar, HOURS), SIGMA_STORE, low_bound, high_bound)
        gen_old, stor_old = gen_now, stor_now
        gen_now, stor_now = gen_next, stor_next
    return gen_now, stor_now, price_level, dual_flow, dual_store
```

```python
import jax
import jax.numpy as jnp
from jax import lax
from jax.sharding import Mesh
from jax.sharding import PartitionSpec as P

HOURS = 24
Z, X, CORES = (8, 4, 2)


TAU = 0.25
SIGMA_FLOW = 4.0
SIGMA_STORE = 0.25
KAPPA = 1.0
THETA = 0.5

AREAS = ("z", "x", "core")
CHIPS = ("z", "x")


def rounded(x):
    return lax.reduce_precision(x, 8, 7)


def swapped(x):
    return lax.ppermute(x, "core", [(0, 1), (1, 0)])


def sum_over_lines(part):
    low = part.astype(jnp.bfloat16)
    near = [
        lax.ppermute(low, "lines", [(i, (i + s) % 4) for i in range(4)]).astype(jnp.float32)
        for s in (1, 2, 3)
    ]
    return (rounded(part) + near[1]) + (near[0] + near[2])


def sent_to_chips(x):
    size = Z * X
    sent = jnp.broadcast_to(x[None], (size, *x.shape))
    return lax.all_to_all(sent, CHIPS, 0, 0, tiled=True)


def gathered_duals(share):
    own = sent_to_chips(share.astype(jnp.bfloat16)).reshape(-1, share.shape[1])
    return own, swapped(own)


def hour_sums(row_count, later):
    row = jnp.arange(row_count, dtype=jnp.int32)
    same = (row[:, None] // HOURS) == (row[None, :] // HOURS)
    side = (row[None, :] >= row[:, None]) if later else (row[None, :] <= row[:, None])
    return jnp.where(same & side, 1.0, 0.0).astype(jnp.float32)


def summed_hours(values, later):
    return jnp.dot(
        hour_sums(values.shape[0], later),
        values,
        precision=lax.Precision.HIGHEST,
        preferred_element_type=jnp.float32,
    )


def dual_step(dual_now, image_term, step_size, low_bound, high_bound):
    shifted = dual_now + step_size * image_term
    return shifted - step_size * jnp.clip(shifted / step_size, low_bound, high_bound)


def shards(
    ptdf,
    load,
    ratings,
    line_index,
    gen_bus,
    gen_quad,
    gen_lin,
    gen_max,
    gen_start,
    stor_bus,
    stor_quad,
    stor_rate,
    stor_energy,
    stor_start,
    lam_start,
    mu_start,
    omega_start,
):
    row_count = load.shape[0]
    line_count, bus_count = ptdf.shape
    gen_count = gen_bus.shape[0]
    stor_count = stor_bus.shape[0]
    area_count = Z * X * CORES
    chip_count = Z * X
    slots = max(8, (gen_count + area_count - 1) // area_count)
    share_len = line_count // area_count
    core = lax.axis_index("core")
    area = (lax.axis_index("z") * X + lax.axis_index("x")) * CORES + core

    target = gen_bus // bus_count
    local_bus = gen_bus % bus_count
    order = jnp.arange(gen_count, dtype=jnp.int32)
    earlier = (target[:, None] == target[None, :]) & (order[None, :] < order[:, None])
    column = target * slots + jnp.sum(earlier.astype(jnp.int32), axis=1)
    slot_of = jnp.arange(area_count * slots, dtype=jnp.int32)
    placed = slot_of[:, None] == column[None, :]
    slot_bus = jnp.sum(jnp.where(placed, local_bus[None, :] + 1, 0), axis=1) - 1
    wanted = lax.all_to_all(slot_bus.reshape(area_count, slots), AREAS, 0, 0, tiled=True)

    dual_flow = mu_start.T
    dual_own, dual_other = gathered_duals(dual_flow)

    bus_ids = jnp.arange(bus_count, dtype=jnp.int32)
    sel_gen = (wanted.reshape(-1)[:, None] == bus_ids[None, :]).astype(jnp.bfloat16)
    sel_stor = (stor_bus[:, None] == bus_ids[None, :]).astype(jnp.bfloat16)
    contract_minor = (((1,), (1,)), ((), ()))
    sent_columns = lax.dot_general(
        sel_gen, ptdf, contract_minor, preferred_element_type=jnp.float32
    ).astype(jnp.bfloat16)
    columns = lax.all_to_all(sent_columns, AREAS, 0, 0, tiled=True)
    weight_stor = lax.dot_general(
        ptdf, sel_stor, contract_minor, preferred_element_type=jnp.float32
    ).astype(jnp.bfloat16)
    pick = (column[:, None] == slot_of[None, :]).astype(jnp.bfloat16)
    weight_gen = lax.dot_general(
        columns, pick, (((0,), (1,)), ((), ())), preferred_element_type=jnp.float32
    ).astype(jnp.bfloat16)
    weight = jnp.concatenate([weight_gen, weight_stor], axis=1)

    def by_core(x):
        split = x.reshape(chip_count, CORES, share_len, x.shape[1])
        own = lax.dynamic_index_in_dim(split, core, 1, keepdims=False)
        other = lax.dynamic_index_in_dim(split, 1 - core, 1, keepdims=False)
        return own.reshape(-1, x.shape[1]), other.reshape(-1, x.shape[1])

    weight_own, weight_other = by_core(weight)
    load_own, load_other = by_core(
        lax.dot_general(
            ptdf, load.astype(jnp.bfloat16), contract_minor, preferred_element_type=jnp.float32
        )
    )
    load_flow = load_own + swapped(load_other)
    load_total = jnp.sum(load, axis=1)

    limit = jnp.take(ratings, lax.dynamic_slice_in_dim(line_index, area * share_len, share_len))[:, None]
    hour_of = jnp.arange(row_count, dtype=jnp.int32) % HOURS
    last_hour = (hour_of == HOURS - 1)[:, None]
    half_energy = (0.5 * stor_energy)[None, :]
    low_bound = jnp.where(last_hour, jnp.zeros_like(half_energy), -half_energy)
    high_bound = jnp.where(last_hour, jnp.zeros_like(half_energy), half_energy)
    total_units = (gen_count + stor_count) * area_count
    gen_now, stor_now = (gen_start, stor_start)
    gen_old, stor_old = (gen_start, stor_start)
    price_level, dual_store = (lam_start, omega_start)
    contract_major = (((0,), (0,)), ((), ()))
    for iteration in range(2):
        if iteration == 0:
            gen_mid, stor_mid = (gen_now, stor_now)
        else:
            gen_mid = gen_now + THETA * (gen_now - gen_old)
            stor_mid = stor_now + THETA * (stor_now - stor_old)
        price = sum_over_lines(
            lax.dot_general(dual_own, weight_own, contract_major, preferred_element_type=jnp.float32)
            + lax.dot_general(dual_other, weight_other, contract_major, preferred_element_type=jnp.float32)
        )
        gen_price, stor_price = price[:, :gen_count], price[:, gen_count:]
        gen_grad = 2.0 * gen_quad * gen_mid + gen_lin + price_level[:, None] + gen_price
        gen_next = jnp.clip(gen_mid - TAU * gen_grad, 0.0, gen_max)
        stor_grad = (
            2.0 * stor_quad * stor_mid
            + price_level[:, None]
            + stor_price
            + summed_hours(dual_store, True)
        )
        stor_next = jnp.clip(stor_mid - TAU * stor_grad, -stor_rate, stor_rate)
        gen_bar = 2.0 * gen_next - gen_now
        stor_bar = 2.0 * stor_next - stor_now
        balance = jnp.sum(gen_bar, axis=1) + jnp.sum(stor_bar, axis=1) - load_total
        bar_low = jnp.concatenate([gen_bar, stor_bar], axis=1).astype(jnp.bfloat16)
        flow_other = lax.dot_general(
            weight_other, bar_low, contract_minor, preferred_element_type=jnp.float32
        )
        flow_own = lax.dot_general(
            weight_own, bar_low, contract_minor, preferred_element_type=jnp.float32
        )
        flow_part = flow_own + swapped(flow_other) - load_flow
        balance = balance + swapped(balance)
        high = rounded(balance)
        lanes = row_count // 3
        tail = jnp.concatenate(
            [
                high.reshape(3, lanes),
                (balance - high).reshape(3, lanes),
                jnp.zeros((share_len - 6, lanes), jnp.float32),
            ],
            axis=0,
        )
        sent = jnp.concatenate(
            [
                flow_part.reshape(chip_count, share_len, row_count),
                jnp.broadcast_to(tail[None], (chip_count, share_len, lanes)),
            ],
            axis=2,
        ).astype(jnp.bfloat16)
        received = lax.all_to_all(sent, CHIPS, 0, 0, tiled=True)
        summed = jnp.sum(received.astype(jnp.float32), axis=0)
        flow_share = summed[:, :row_count]
        balance = (summed[:3, row_count:] + summed[3:6, row_count:]).reshape(row_count)
        dual_flow = dual_step(dual_flow, flow_share, SIGMA_FLOW, -limit, limit)
        if iteration == 0:
            dual_own, dual_other = gathered_duals(dual_flow)
        price_level = price_level + KAPPA / total_units * balance
        dual_store = dual_step(
            dual_store, summed_hours(stor_bar, False), SIGMA_STORE, low_bound, high_bound
        )
        gen_old, stor_old = (gen_now, stor_now)
        gen_now, stor_now = (gen_next, stor_next)
    return (gen_now, stor_now, price_level, dual_flow.T, dual_store)


def solution(mesh):
    fine = Mesh(
        mesh.devices.reshape(mesh.shape["lines"], Z, X, CORES), ("lines", "z", "x", "core")
    )
    by_area = P(AREAS)
    by_column = P(None, AREAS)
    return jax.shard_map(
        shards,
        mesh=fine,
        in_specs=(
            P("lines", AREAS),
            by_column,
            P(),
            P("lines"),
            by_area,
            by_area,
            by_area,
            by_area,
            by_column,
            by_area,
            by_area,
            by_area,
            by_area,
            by_column,
            P(),
            P(None, ("lines", *AREAS)),
            by_column,
        ),
        out_specs=(by_column, by_column, P(), P(None, ("lines", *AREAS)), by_column),
        check_vma=False,
    )
```

```python
import jax
import jax.numpy as jnp
from jax import lax
from jax.sharding import Mesh
from jax.sharding import PartitionSpec as P

HOURS = 24
Z, X, CORES = (8, 4, 2)


TAU = 0.25
SIGMA_FLOW = 4.0
SIGMA_STORE = 0.25
KAPPA = 1.0
THETA = 0.5

AREAS = ("z", "x", "core")
CHIPS = ("z", "x")


def rounded(x):
    return lax.reduce_precision(x, 8, 7)


def swapped(x):
    return lax.ppermute(x, "core", [(0, 1), (1, 0)])


def sum_over_lines(part):
    low = part.astype(jnp.bfloat16)
    near = [
        lax.ppermute(low, "lines", [(i, (i + s) % 4) for i in range(4)]).astype(jnp.float32)
        for s in (1, 2, 3)
    ]
    return (rounded(part) + near[1]) + (near[0] + near[2])


def sent_to_chips(x):
    size = Z * X
    sent = jnp.broadcast_to(x[None], (size, *x.shape))
    return lax.all_to_all(sent, CHIPS, 0, 0, tiled=True)


def gathered_duals(share):
    own = sent_to_chips(share.astype(jnp.bfloat16)).reshape(-1, share.shape[1])
    return own, swapped(own)


def doubled(x, axis, size, step, dim):
    other = lax.ppermute(x, axis, [(i, i ^ step) for i in range(size)])
    first = (lax.axis_index(axis) // step) % 2 == 0
    return jnp.where(
        first, jnp.concatenate([x, other], axis=dim), jnp.concatenate([other, x], axis=dim)
    )


def gathered_early(share):
    share_len, row_count = share.shape
    held = share.astype(jnp.bfloat16).reshape(1, 1, share_len, row_count)
    for step in (1, 2, 4):
        held = doubled(held, "z", Z, step, 0)
    for step in (1, 2):
        held = doubled(held, "x", X, step, 1)
    own = held.reshape(-1, row_count)
    return own, swapped(own)


def hour_sums(row_count, later):
    row = jnp.arange(row_count, dtype=jnp.int32)
    same = (row[:, None] // HOURS) == (row[None, :] // HOURS)
    side = (row[None, :] >= row[:, None]) if later else (row[None, :] <= row[:, None])
    return jnp.where(same & side, 1.0, 0.0).astype(jnp.float32)


def summed_hours(values, later):
    return jnp.dot(
        hour_sums(values.shape[0], later),
        values,
        precision=lax.Precision.HIGHEST,
        preferred_element_type=jnp.float32,
    )


def dual_step(dual_now, image_term, step_size, low_bound, high_bound):
    shifted = dual_now + step_size * image_term
    return shifted - step_size * jnp.clip(shifted / step_size, low_bound, high_bound)


def shards(
    ptdf,
    load,
    ratings,
    line_index,
    gen_bus,
    gen_quad,
    gen_lin,
    gen_max,
    gen_start,
    stor_bus,
    stor_quad,
    stor_rate,
    stor_energy,
    stor_start,
    lam_start,
    mu_start,
    omega_start,
):
    row_count = load.shape[0]
    line_count, bus_count = ptdf.shape
    gen_count = gen_bus.shape[0]
    stor_count = stor_bus.shape[0]
    area_count = Z * X * CORES
    chip_count = Z * X
    slots = max(8, (gen_count + area_count - 1) // area_count)
    share_len = line_count // area_count
    core = lax.axis_index("core")
    area = (lax.axis_index("z") * X + lax.axis_index("x")) * CORES + core

    target = gen_bus // bus_count
    local_bus = gen_bus % bus_count
    order = jnp.arange(gen_count, dtype=jnp.int32)
    earlier = (target[:, None] == target[None, :]) & (order[None, :] < order[:, None])
    column = target * slots + jnp.sum(earlier.astype(jnp.int32), axis=1)
    slot_of = jnp.arange(area_count * slots, dtype=jnp.int32)
    placed = slot_of[:, None] == column[None, :]
    slot_bus = jnp.sum(jnp.where(placed, local_bus[None, :] + 1, 0), axis=1) - 1
    wanted = lax.all_to_all(slot_bus.reshape(area_count, slots), AREAS, 0, 0, tiled=True)

    dual_flow = mu_start.T
    dual_own, dual_other = gathered_early(dual_flow)

    bus_ids = jnp.arange(bus_count, dtype=jnp.int32)
    sel_gen = (wanted.reshape(-1)[:, None] == bus_ids[None, :]).astype(jnp.bfloat16)
    sel_stor = (stor_bus[:, None] == bus_ids[None, :]).astype(jnp.bfloat16)
    contract_minor = (((1,), (1,)), ((), ()))
    sent_columns = lax.dot_general(
        sel_gen, ptdf, contract_minor, preferred_element_type=jnp.float32
    ).astype(jnp.bfloat16)
    columns = lax.all_to_all(sent_columns, AREAS, 0, 0, tiled=True)
    weight_stor = lax.dot_general(
        ptdf, sel_stor, contract_minor, preferred_element_type=jnp.float32
    ).astype(jnp.bfloat16)
    pick = (column[:, None] == slot_of[None, :]).astype(jnp.bfloat16)
    weight_gen = lax.dot_general(
        columns, pick, (((0,), (1,)), ((), ())), preferred_element_type=jnp.float32
    ).astype(jnp.bfloat16)
    weight = jnp.concatenate([weight_gen, weight_stor], axis=1)

    def by_core(x):
        split = x.reshape(chip_count, CORES, share_len, x.shape[1])
        own = lax.dynamic_index_in_dim(split, core, 1, keepdims=False)
        other = lax.dynamic_index_in_dim(split, 1 - core, 1, keepdims=False)
        return own.reshape(-1, x.shape[1]), other.reshape(-1, x.shape[1])

    weight_own, weight_other = by_core(weight)
    load_own, load_other = by_core(
        lax.dot_general(
            ptdf, load.astype(jnp.bfloat16), contract_minor, preferred_element_type=jnp.float32
        )
    )
    load_flow = load_own + swapped(load_other)
    load_total = jnp.sum(load, axis=1)

    limit = jnp.take(ratings, lax.dynamic_slice_in_dim(line_index, area * share_len, share_len))[:, None]
    hour_of = jnp.arange(row_count, dtype=jnp.int32) % HOURS
    last_hour = (hour_of == HOURS - 1)[:, None]
    half_energy = (0.5 * stor_energy)[None, :]
    low_bound = jnp.where(last_hour, jnp.zeros_like(half_energy), -half_energy)
    high_bound = jnp.where(last_hour, jnp.zeros_like(half_energy), half_energy)
    total_units = (gen_count + stor_count) * area_count
    gen_now, stor_now = (gen_start, stor_start)
    gen_old, stor_old = (gen_start, stor_start)
    price_level, dual_store = (lam_start, omega_start)
    contract_major = (((0,), (0,)), ((), ()))
    for iteration in range(2):
        if iteration == 0:
            gen_mid, stor_mid = (gen_now, stor_now)
        else:
            gen_mid = gen_now + THETA * (gen_now - gen_old)
            stor_mid = stor_now + THETA * (stor_now - stor_old)
        price = sum_over_lines(
            lax.dot_general(dual_own, weight_own, contract_major, preferred_element_type=jnp.float32)
            + lax.dot_general(dual_other, weight_other, contract_major, preferred_element_type=jnp.float32)
        )
        gen_price, stor_price = price[:, :gen_count], price[:, gen_count:]
        gen_grad = 2.0 * gen_quad * gen_mid + gen_lin + price_level[:, None] + gen_price
        gen_next = jnp.clip(gen_mid - TAU * gen_grad, 0.0, gen_max)
        stor_grad = (
            2.0 * stor_quad * stor_mid
            + price_level[:, None]
            + stor_price
            + summed_hours(dual_store, True)
        )
        stor_next = jnp.clip(stor_mid - TAU * stor_grad, -stor_rate, stor_rate)
        gen_bar = 2.0 * gen_next - gen_now
        stor_bar = 2.0 * stor_next - stor_now
        balance = jnp.sum(gen_bar, axis=1) + jnp.sum(stor_bar, axis=1) - load_total
        bar_low = jnp.concatenate([gen_bar, stor_bar], axis=1).astype(jnp.bfloat16)
        flow_other = lax.dot_general(
            weight_other, bar_low, contract_minor, preferred_element_type=jnp.float32
        )
        flow_own = lax.dot_general(
            weight_own, bar_low, contract_minor, preferred_element_type=jnp.float32
        )
        flow_part = flow_own + swapped(flow_other) - load_flow
        balance = balance + swapped(balance)
        high = rounded(balance)
        lanes = row_count // 3
        tail = jnp.concatenate(
            [
                high.reshape(3, lanes),
                (balance - high).reshape(3, lanes),
                jnp.zeros((share_len - 6, lanes), jnp.float32),
            ],
            axis=0,
        )
        sent = jnp.concatenate(
            [
                flow_part.reshape(chip_count, share_len, row_count),
                jnp.broadcast_to(tail[None], (chip_count, share_len, lanes)),
            ],
            axis=2,
        ).astype(jnp.bfloat16)
        received = lax.all_to_all(sent, CHIPS, 0, 0, tiled=True)
        summed = jnp.sum(received.astype(jnp.float32), axis=0)
        flow_share = summed[:, :row_count]
        balance = (summed[:3, row_count:] + summed[3:6, row_count:]).reshape(row_count)
        dual_flow = dual_step(dual_flow, flow_share, SIGMA_FLOW, -limit, limit)
        if iteration == 0:
            dual_own, dual_other = gathered_duals(dual_flow)
        price_level = price_level + KAPPA / total_units * balance
        dual_store = dual_step(
            dual_store, summed_hours(stor_bar, False), SIGMA_STORE, low_bound, high_bound
        )
        gen_old, stor_old = (gen_now, stor_now)
        gen_now, stor_now = (gen_next, stor_next)
    return (gen_now, stor_now, price_level, dual_flow.T, dual_store)


def solution(mesh):
    fine = Mesh(
        mesh.devices.reshape(mesh.shape["lines"], Z, X, CORES), ("lines", "z", "x", "core")
    )
    by_area = P(AREAS)
    by_column = P(None, AREAS)
    return jax.shard_map(
        shards,
        mesh=fine,
        in_specs=(
            P("lines", AREAS),
            by_column,
            P(),
            P("lines"),
            by_area,
            by_area,
            by_area,
            by_area,
            by_column,
            by_area,
            by_area,
            by_area,
            by_area,
            by_column,
            P(),
            P(None, ("lines", *AREAS)),
            by_column,
        ),
        out_specs=(by_column, by_column, P(), P(None, ("lines", *AREAS)), by_column),
        check_vma=False,
    )
```

```python
import jax
import jax.numpy as jnp
from jax import lax
from jax.sharding import Mesh
from jax.sharding import PartitionSpec as P

HOURS = 24
Z, X, CORES = (8, 4, 2)


TAU = 0.25
SIGMA_FLOW = 4.0
SIGMA_STORE = 0.25
KAPPA = 1.0
THETA = 0.5

AREAS = ("z", "x", "core")
CHIPS = ("z", "x")


def rounded(x):
    return lax.reduce_precision(x, 8, 7)


def swapped(x):
    return lax.ppermute(x, "core", [(0, 1), (1, 0)])


def sum_over_lines(part):
    low = part.astype(jnp.bfloat16)
    near = [
        lax.ppermute(low, "lines", [(i, (i + s) % 4) for i in range(4)]).astype(jnp.float32)
        for s in (1, 2, 3)
    ]
    return (rounded(part) + near[1]) + (near[0] + near[2])


def sent_to_chips(x):
    size = Z * X
    sent = jnp.broadcast_to(x[None], (size, *x.shape))
    return lax.all_to_all(sent, CHIPS, 0, 0, tiled=True)


def gathered_duals(share):
    own = sent_to_chips(share.astype(jnp.bfloat16)).reshape(-1, share.shape[1])
    return own, swapped(own)


def doubled(x, axis, size, step, dim):
    other = lax.ppermute(x, axis, [(i, i ^ step) for i in range(size)])
    first = (lax.axis_index(axis) // step) % 2 == 0
    return jnp.where(
        first, jnp.concatenate([x, other], axis=dim), jnp.concatenate([other, x], axis=dim)
    )


def gathered_early(share):
    share_len, row_count = share.shape
    held = share.astype(jnp.bfloat16).reshape(1, 1, share_len, row_count)
    for step in (1, 2, 4):
        held = doubled(held, "z", Z, step, 0)
    near = [held]
    for step in (1, 2, 3):
        near.append(lax.ppermute(held, "x", [(i, i ^ step) for i in range(X)]))
    index = lax.axis_index("x")
    low, high = index % 2 == 0, index // 2 == 0

    def pair(first, second):
        return jnp.where(
            low,
            jnp.concatenate([first, second], axis=1),
            jnp.concatenate([second, first], axis=1),
        )

    mine, far = pair(near[0], near[1]), pair(near[2], near[3])
    held = jnp.where(
        high, jnp.concatenate([mine, far], axis=1), jnp.concatenate([far, mine], axis=1)
    )
    own = held.reshape(-1, row_count)
    return own, swapped(own)


def hour_sums(row_count, later):
    row = jnp.arange(row_count, dtype=jnp.int32)
    same = (row[:, None] // HOURS) == (row[None, :] // HOURS)
    side = (row[None, :] >= row[:, None]) if later else (row[None, :] <= row[:, None])
    return jnp.where(same & side, 1.0, 0.0).astype(jnp.float32)


def summed_hours(values, later):
    return jnp.dot(
        hour_sums(values.shape[0], later),
        values,
        precision=lax.Precision.HIGHEST,
        preferred_element_type=jnp.float32,
    )


def dual_step(dual_now, image_term, step_size, low_bound, high_bound):
    shifted = dual_now + step_size * image_term
    return shifted - step_size * jnp.clip(shifted / step_size, low_bound, high_bound)


def shards(
    ptdf,
    load,
    ratings,
    line_index,
    gen_bus,
    gen_quad,
    gen_lin,
    gen_max,
    gen_start,
    stor_bus,
    stor_quad,
    stor_rate,
    stor_energy,
    stor_start,
    lam_start,
    mu_start,
    omega_start,
):
    row_count = load.shape[0]
    line_count, bus_count = ptdf.shape
    gen_count = gen_bus.shape[0]
    stor_count = stor_bus.shape[0]
    area_count = Z * X * CORES
    chip_count = Z * X
    slots = max(8, (gen_count + area_count - 1) // area_count)
    share_len = line_count // area_count
    core = lax.axis_index("core")
    area = (lax.axis_index("z") * X + lax.axis_index("x")) * CORES + core

    target = gen_bus // bus_count
    local_bus = gen_bus % bus_count
    order = jnp.arange(gen_count, dtype=jnp.int32)
    earlier = (target[:, None] == target[None, :]) & (order[None, :] < order[:, None])
    column = target * slots + jnp.sum(earlier.astype(jnp.int32), axis=1)
    slot_of = jnp.arange(area_count * slots, dtype=jnp.int32)
    placed = slot_of[:, None] == column[None, :]
    slot_bus = jnp.sum(jnp.where(placed, local_bus[None, :] + 1, 0), axis=1) - 1
    wanted = lax.all_to_all(slot_bus.reshape(area_count, slots), AREAS, 0, 0, tiled=True)

    dual_flow = mu_start.T
    dual_own, dual_other = gathered_early(dual_flow)

    bus_ids = jnp.arange(bus_count, dtype=jnp.int32)
    sel_gen = (wanted.reshape(-1)[:, None] == bus_ids[None, :]).astype(jnp.bfloat16)
    sel_stor = (stor_bus[:, None] == bus_ids[None, :]).astype(jnp.bfloat16)
    contract_minor = (((1,), (1,)), ((), ()))
    sent_columns = lax.dot_general(
        sel_gen, ptdf, contract_minor, preferred_element_type=jnp.float32
    ).astype(jnp.bfloat16)
    columns = lax.all_to_all(sent_columns, AREAS, 0, 0, tiled=True)
    weight_stor = lax.dot_general(
        ptdf, sel_stor, contract_minor, preferred_element_type=jnp.float32
    ).astype(jnp.bfloat16)
    pick = (column[:, None] == slot_of[None, :]).astype(jnp.bfloat16)
    weight_gen = lax.dot_general(
        columns, pick, (((0,), (1,)), ((), ())), preferred_element_type=jnp.float32
    ).astype(jnp.bfloat16)
    weight = jnp.concatenate([weight_gen, weight_stor], axis=1)

    def by_core(x):
        split = x.reshape(chip_count, CORES, share_len, x.shape[1])
        own = lax.dynamic_index_in_dim(split, core, 1, keepdims=False)
        other = lax.dynamic_index_in_dim(split, 1 - core, 1, keepdims=False)
        return own.reshape(-1, x.shape[1]), other.reshape(-1, x.shape[1])

    weight_own, weight_other = by_core(weight)
    load_own, load_other = by_core(
        lax.dot_general(
            ptdf, load.astype(jnp.bfloat16), contract_minor, preferred_element_type=jnp.float32
        )
    )
    load_flow = load_own + swapped(load_other)
    load_total = jnp.sum(load, axis=1)

    limit = jnp.take(ratings, lax.dynamic_slice_in_dim(line_index, area * share_len, share_len))[:, None]
    hour_of = jnp.arange(row_count, dtype=jnp.int32) % HOURS
    last_hour = (hour_of == HOURS - 1)[:, None]
    half_energy = (0.5 * stor_energy)[None, :]
    low_bound = jnp.where(last_hour, jnp.zeros_like(half_energy), -half_energy)
    high_bound = jnp.where(last_hour, jnp.zeros_like(half_energy), half_energy)
    total_units = (gen_count + stor_count) * area_count
    gen_now, stor_now = (gen_start, stor_start)
    gen_old, stor_old = (gen_start, stor_start)
    price_level, dual_store = (lam_start, omega_start)
    contract_major = (((0,), (0,)), ((), ()))
    for iteration in range(2):
        if iteration == 0:
            gen_mid, stor_mid = (gen_now, stor_now)
        else:
            gen_mid = gen_now + THETA * (gen_now - gen_old)
            stor_mid = stor_now + THETA * (stor_now - stor_old)
        price = sum_over_lines(
            lax.dot_general(dual_own, weight_own, contract_major, preferred_element_type=jnp.float32)
            + lax.dot_general(dual_other, weight_other, contract_major, preferred_element_type=jnp.float32)
        )
        gen_price, stor_price = price[:, :gen_count], price[:, gen_count:]
        gen_grad = 2.0 * gen_quad * gen_mid + gen_lin + price_level[:, None] + gen_price
        gen_next = jnp.clip(gen_mid - TAU * gen_grad, 0.0, gen_max)
        stor_grad = (
            2.0 * stor_quad * stor_mid
            + price_level[:, None]
            + stor_price
            + summed_hours(dual_store, True)
        )
        stor_next = jnp.clip(stor_mid - TAU * stor_grad, -stor_rate, stor_rate)
        gen_bar = 2.0 * gen_next - gen_now
        stor_bar = 2.0 * stor_next - stor_now
        balance = jnp.sum(gen_bar, axis=1) + jnp.sum(stor_bar, axis=1) - load_total
        bar_low = jnp.concatenate([gen_bar, stor_bar], axis=1).astype(jnp.bfloat16)
        flow_other = lax.dot_general(
            weight_other, bar_low, contract_minor, preferred_element_type=jnp.float32
        )
        flow_own = lax.dot_general(
            weight_own, bar_low, contract_minor, preferred_element_type=jnp.float32
        )
        flow_part = flow_own + swapped(flow_other) - load_flow
        balance = balance + swapped(balance)
        high = rounded(balance)
        lanes = 128
        strips = row_count // lanes
        tail = jnp.concatenate(
            [
                high.reshape(strips, lanes),
                (balance - high).reshape(strips, lanes),
                jnp.zeros((8 - 2 * strips, lanes), jnp.float32),
            ],
            axis=0,
        )
        body = flow_part.reshape(chip_count, share_len, row_count)
        sent = jnp.concatenate(
            [body[:, :, i * lanes : (i + 1) * lanes] for i in range(strips)]
            + [jnp.broadcast_to(tail[None], (chip_count, 8, lanes))],
            axis=1,
        ).astype(jnp.bfloat16)
        received = lax.all_to_all(sent, CHIPS, 0, 0, tiled=True)
        summed = jnp.sum(received.astype(jnp.float32), axis=0)
        flow_share = jnp.concatenate(
            [summed[i * share_len : (i + 1) * share_len] for i in range(strips)], axis=1
        )
        tail = summed[strips * share_len :]
        balance = (tail[:strips] + tail[strips : 2 * strips]).reshape(row_count)
        dual_flow = dual_step(dual_flow, flow_share, SIGMA_FLOW, -limit, limit)
        if iteration == 0:
            dual_own, dual_other = gathered_duals(dual_flow)
        price_level = price_level + KAPPA / total_units * balance
        dual_store = dual_step(
            dual_store, summed_hours(stor_bar, False), SIGMA_STORE, low_bound, high_bound
        )
        gen_old, stor_old = (gen_now, stor_now)
        gen_now, stor_now = (gen_next, stor_next)
    return (gen_now, stor_now, price_level, dual_flow.T, dual_store)


def solution(mesh):
    fine = Mesh(
        mesh.devices.reshape(mesh.shape["lines"], Z, X, CORES), ("lines", "z", "x", "core")
    )
    by_area = P(AREAS)
    by_column = P(None, AREAS)
    return jax.shard_map(
        shards,
        mesh=fine,
        in_specs=(
            P("lines", AREAS),
            by_column,
            P(),
            P("lines"),
            by_area,
            by_area,
            by_area,
            by_area,
            by_column,
            by_area,
            by_area,
            by_area,
            by_area,
            by_column,
            P(),
            P(None, ("lines", *AREAS)),
            by_column,
        ),
        out_specs=(by_column, by_column, P(), P(None, ("lines", *AREAS)), by_column),
        check_vma=False,
    )
```

```python
import jax
import jax.numpy as jnp
from jax import lax
from jax.experimental import pallas as pl
from jax.experimental.pallas import tpu as pltpu
from jax.sharding import Mesh
from jax.sharding import PartitionSpec as P

HOURS = 24
Z, X, CORES = (8, 4, 2)


TAU = 0.25
SIGMA_FLOW = 4.0
SIGMA_STORE = 0.25
KAPPA = 1.0
THETA = 0.5

AREAS = ("z", "x", "core")
CHIPS = ("z", "x")


def rounded(x):
    return lax.reduce_precision(x, 8, 7)


def swapped(x):
    return lax.ppermute(x, "core", [(0, 1), (1, 0)])


CONTRACT_MAJOR = (((0,), (0,)), ((), ()))
CONTRACT_MINOR = (((1,), (1,)), ((), ()))


def with_side(x, step):
    other = lax.ppermute(x.astype(jnp.bfloat16), "lines", [(i, i ^ step) for i in range(4)])
    return x + other.astype(jnp.float32)


def sum_over_lines(halves):
    first, second = (rounded(half.astype(jnp.float32)) for half in halves)
    first, second = rounded(with_side(first, 1)), rounded(with_side(second, 3))
    return jnp.concatenate([with_side(first, 3), with_side(second, 1)], axis=0)


def store_price(dual_own, dual_other, weight_own, weight_other, first, second):
    price = lax.dot_general(
        dual_own[...], weight_own[...], CONTRACT_MAJOR, preferred_element_type=jnp.float32
    ) + lax.dot_general(
        dual_other[...], weight_other[...], CONTRACT_MAJOR, preferred_element_type=jnp.float32
    )
    rows = first.shape[0]
    first[...] = price[:rows].astype(jnp.bfloat16)
    second[...] = price[rows:].astype(jnp.bfloat16)


def weights_body(
    core,
    columns,
    column,
    stor_own,
    stor_other,
    dual_own,
    dual_other,
    weight_own,
    weight_other,
    first,
    second,
    split,
):
    slot_count, gen_count = columns.shape[0], column.shape[1]
    slot = lax.broadcasted_iota(jnp.int32, (slot_count, gen_count), 0)
    pick = jnp.where(slot == column[...], 1.0, 0.0).astype(jnp.bfloat16)
    weight = lax.dot_general(
        columns[...], pick, CONTRACT_MAJOR, preferred_element_type=jnp.float32
    )
    split[...] = weight.astype(jnp.bfloat16).reshape(split.shape)
    share_len = split.shape[1]
    mine = core[0]
    for chip in range(split.shape[0] // CORES):
        rows = slice(chip * share_len, (chip + 1) * share_len)
        weight_own[rows, :gen_count] = split[CORES * chip + mine]
        weight_other[rows, :gen_count] = split[CORES * chip + 1 - mine]
    weight_own[:, gen_count:] = stor_own[...]
    weight_other[:, gen_count:] = stor_other[...]
    store_price(dual_own, dual_other, weight_own, weight_other, first, second)


def price_body(dual_own, dual_other, weight_own, weight_other, first, second):
    store_price(dual_own, dual_other, weight_own, weight_other, first, second)


def half_prices(row_count, units):
    half = jax.ShapeDtypeStruct((row_count // 2, units), jnp.bfloat16)
    return (half, half)


def weights_and_prices(core, columns, column, stor_own, stor_other, dual_own, dual_other):
    half_lines, row_count = dual_own.shape
    gen_count = column.shape[0]
    units = gen_count + stor_own.shape[1]
    weight = jax.ShapeDtypeStruct((half_lines, units), jnp.bfloat16)
    in_vmem = pl.BlockSpec(memory_space=pltpu.VMEM)
    share_len = columns.shape[1] // (Z * X * CORES)
    own, other, first, second = pl.pallas_call(
        weights_body,
        out_shape=(weight, weight, *half_prices(row_count, units)),
        in_specs=[pl.BlockSpec(memory_space=pltpu.SMEM)] + [in_vmem] * 6,
        out_specs=(in_vmem,) * 4,
        scratch_shapes=[pltpu.VMEM((Z * X * CORES, share_len, gen_count), jnp.bfloat16)],
        name="weights",
    )(core.reshape(1), columns, column.reshape(1, -1), stor_own, stor_other, dual_own, dual_other)
    return own, other, (first, second)


def later_prices(dual_own, dual_other, weight_own, weight_other):
    in_vmem = pl.BlockSpec(memory_space=pltpu.VMEM)
    return pl.pallas_call(
        price_body,
        out_shape=half_prices(dual_own.shape[1], weight_own.shape[1]),
        in_specs=[in_vmem] * 4,
        out_specs=(in_vmem,) * 2,
        name="prices",
    )(dual_own, dual_other, weight_own, weight_other)


def sent_to_chips(x):
    size = Z * X
    sent = jnp.broadcast_to(x[None], (size, *x.shape))
    return lax.all_to_all(sent, CHIPS, 0, 0, tiled=True)


def gathered_duals(share):
    own = sent_to_chips(share.astype(jnp.bfloat16)).reshape(-1, share.shape[1])
    return own, swapped(own)


def doubled(x, axis, size, step, dim):
    other = lax.ppermute(x, axis, [(i, i ^ step) for i in range(size)])
    first = (lax.axis_index(axis) // step) % 2 == 0
    return jnp.where(
        first, jnp.concatenate([x, other], axis=dim), jnp.concatenate([other, x], axis=dim)
    )


def gathered_early(share):
    share_len, row_count = share.shape
    held = share.astype(jnp.bfloat16).reshape(1, 1, share_len, row_count)
    for step in (1, 2, 4):
        held = doubled(held, "z", Z, step, 0)
    near = [held]
    for step in (1, 2, 3):
        near.append(lax.ppermute(held, "x", [(i, i ^ step) for i in range(X)]))
    index = lax.axis_index("x")
    low, high = index % 2 == 0, index // 2 == 0

    def pair(first, second):
        return jnp.where(
            low,
            jnp.concatenate([first, second], axis=1),
            jnp.concatenate([second, first], axis=1),
        )

    mine, far = pair(near[0], near[1]), pair(near[2], near[3])
    held = jnp.where(
        high, jnp.concatenate([mine, far], axis=1), jnp.concatenate([far, mine], axis=1)
    )
    own = held.reshape(-1, row_count)
    return own, swapped(own)


def hour_sums(row_count, later):
    row = jnp.arange(row_count, dtype=jnp.int32)
    same = (row[:, None] // HOURS) == (row[None, :] // HOURS)
    side = (row[None, :] >= row[:, None]) if later else (row[None, :] <= row[:, None])
    return jnp.where(same & side, 1.0, 0.0).astype(jnp.float32)


def summed_hours(values, later):
    return jnp.dot(
        hour_sums(values.shape[0], later),
        values,
        precision=lax.Precision.HIGHEST,
        preferred_element_type=jnp.float32,
    )


def dual_step(dual_now, image_term, step_size, low_bound, high_bound):
    shifted = dual_now + step_size * image_term
    return shifted - step_size * jnp.clip(shifted / step_size, low_bound, high_bound)


def shards(
    ptdf,
    load,
    ratings,
    line_index,
    gen_bus,
    gen_quad,
    gen_lin,
    gen_max,
    gen_start,
    stor_bus,
    stor_quad,
    stor_rate,
    stor_energy,
    stor_start,
    lam_start,
    mu_start,
    omega_start,
):
    row_count = load.shape[0]
    line_count, bus_count = ptdf.shape
    gen_count = gen_bus.shape[0]
    stor_count = stor_bus.shape[0]
    area_count = Z * X * CORES
    chip_count = Z * X
    slots = max(8, (gen_count + area_count - 1) // area_count)
    share_len = line_count // area_count
    core = lax.axis_index("core")
    area = (lax.axis_index("z") * X + lax.axis_index("x")) * CORES + core

    target = gen_bus // bus_count
    local_bus = gen_bus % bus_count
    order = jnp.arange(gen_count, dtype=jnp.int32)
    earlier = (target[:, None] == target[None, :]) & (order[None, :] < order[:, None])
    column = target * slots + jnp.sum(earlier.astype(jnp.int32), axis=1)
    slot_of = jnp.arange(area_count * slots, dtype=jnp.int32)
    placed = slot_of[:, None] == column[None, :]
    slot_bus = jnp.sum(jnp.where(placed, local_bus[None, :] + 1, 0), axis=1) - 1
    wanted = lax.all_to_all(slot_bus.reshape(area_count, slots), AREAS, 0, 0, tiled=True)

    dual_flow = mu_start.T
    dual_own, dual_other = gathered_early(dual_flow)

    bus_ids = jnp.arange(bus_count, dtype=jnp.int32)
    sel_gen = (wanted.reshape(-1)[:, None] == bus_ids[None, :]).astype(jnp.bfloat16)
    sel_stor = (stor_bus[:, None] == bus_ids[None, :]).astype(jnp.bfloat16)
    sent_columns = lax.dot_general(
        sel_gen, ptdf, CONTRACT_MINOR, preferred_element_type=jnp.float32
    ).astype(jnp.bfloat16)
    columns = lax.all_to_all(sent_columns, AREAS, 0, 0, tiled=True)
    weight_stor = lax.dot_general(
        ptdf, sel_stor, CONTRACT_MINOR, preferred_element_type=jnp.float32
    ).astype(jnp.bfloat16)

    def by_core(x):
        split = x.reshape(chip_count, CORES, share_len, x.shape[1])
        own = lax.dynamic_index_in_dim(split, core, 1, keepdims=False)
        other = lax.dynamic_index_in_dim(split, 1 - core, 1, keepdims=False)
        return own.reshape(-1, x.shape[1]), other.reshape(-1, x.shape[1])

    weight_own, weight_other, halves = weights_and_prices(
        core,
        columns.reshape(-1, line_count),
        column,
        *by_core(weight_stor),
        dual_own,
        dual_other,
    )
    load_own, load_other = by_core(
        lax.dot_general(
            ptdf, load.astype(jnp.bfloat16), CONTRACT_MINOR, preferred_element_type=jnp.float32
        )
    )
    load_flow = load_own + swapped(load_other)
    load_total = jnp.sum(load, axis=1)

    limit = jnp.take(ratings, lax.dynamic_slice_in_dim(line_index, area * share_len, share_len))[:, None]
    hour_of = jnp.arange(row_count, dtype=jnp.int32) % HOURS
    last_hour = (hour_of == HOURS - 1)[:, None]
    half_energy = (0.5 * stor_energy)[None, :]
    low_bound = jnp.where(last_hour, jnp.zeros_like(half_energy), -half_energy)
    high_bound = jnp.where(last_hour, jnp.zeros_like(half_energy), half_energy)
    total_units = (gen_count + stor_count) * area_count
    gen_now, stor_now = (gen_start, stor_start)
    gen_old, stor_old = (gen_start, stor_start)
    price_level, dual_store = (lam_start, omega_start)
    for iteration in range(2):
        if iteration == 0:
            gen_mid, stor_mid = (gen_now, stor_now)
        else:
            gen_mid = gen_now + THETA * (gen_now - gen_old)
            stor_mid = stor_now + THETA * (stor_now - stor_old)
        if iteration > 0:
            halves = later_prices(dual_own, dual_other, weight_own, weight_other)
        price = sum_over_lines(halves)
        gen_price, stor_price = price[:, :gen_count], price[:, gen_count:]
        gen_grad = 2.0 * gen_quad * gen_mid + gen_lin + price_level[:, None] + gen_price
        gen_next = jnp.clip(gen_mid - TAU * gen_grad, 0.0, gen_max)
        stor_grad = (
            2.0 * stor_quad * stor_mid
            + price_level[:, None]
            + stor_price
            + summed_hours(dual_store, True)
        )
        stor_next = jnp.clip(stor_mid - TAU * stor_grad, -stor_rate, stor_rate)
        gen_bar = 2.0 * gen_next - gen_now
        stor_bar = 2.0 * stor_next - stor_now
        balance = jnp.sum(gen_bar, axis=1) + jnp.sum(stor_bar, axis=1) - load_total
        bar_low = jnp.concatenate([gen_bar, stor_bar], axis=1).astype(jnp.bfloat16)
        flow_other = lax.dot_general(
            weight_other, bar_low, CONTRACT_MINOR, preferred_element_type=jnp.float32
        )
        flow_own = lax.dot_general(
            weight_own, bar_low, CONTRACT_MINOR, preferred_element_type=jnp.float32
        )
        flow_part = flow_own + swapped(flow_other) - load_flow
        balance = balance + swapped(balance)
        high = rounded(balance)
        lanes = 128
        strips = row_count // lanes
        tail = jnp.concatenate(
            [
                high.reshape(strips, lanes),
                (balance - high).reshape(strips, lanes),
                jnp.zeros((8 - 2 * strips, lanes), jnp.float32),
            ],
            axis=0,
        )
        body = flow_part.reshape(chip_count, share_len, row_count)
        sent = jnp.concatenate(
            [body[:, :, i * lanes : (i + 1) * lanes] for i in range(strips)]
            + [jnp.broadcast_to(tail[None], (chip_count, 8, lanes))],
            axis=1,
        ).astype(jnp.bfloat16)
        received = lax.all_to_all(sent, CHIPS, 0, 0, tiled=True)
        summed = jnp.sum(received.astype(jnp.float32), axis=0)
        flow_share = jnp.concatenate(
            [summed[i * share_len : (i + 1) * share_len] for i in range(strips)], axis=1
        )
        tail = summed[strips * share_len :]
        balance = (tail[:strips] + tail[strips : 2 * strips]).reshape(row_count)
        dual_flow = dual_step(dual_flow, flow_share, SIGMA_FLOW, -limit, limit)
        if iteration == 0:
            dual_own, dual_other = gathered_duals(dual_flow)
        price_level = price_level + KAPPA / total_units * balance
        dual_store = dual_step(
            dual_store, summed_hours(stor_bar, False), SIGMA_STORE, low_bound, high_bound
        )
        gen_old, stor_old = (gen_now, stor_now)
        gen_now, stor_now = (gen_next, stor_next)
    return (gen_now, stor_now, price_level, dual_flow.T, dual_store)


def solution(mesh):
    fine = Mesh(
        mesh.devices.reshape(mesh.shape["lines"], Z, X, CORES), ("lines", "z", "x", "core")
    )
    by_area = P(AREAS)
    by_column = P(None, AREAS)
    return jax.shard_map(
        shards,
        mesh=fine,
        in_specs=(
            P("lines", AREAS),
            by_column,
            P(),
            P("lines"),
            by_area,
            by_area,
            by_area,
            by_area,
            by_column,
            by_area,
            by_area,
            by_area,
            by_area,
            by_column,
            P(),
            P(None, ("lines", *AREAS)),
            by_column,
        ),
        out_specs=(by_column, by_column, P(), P(None, ("lines", *AREAS)), by_column),
        check_vma=False,
    )
```

```python
import jax
import jax.numpy as jnp
from jax import lax
from jax.experimental import pallas as pl
from jax.experimental.pallas import tpu as pltpu
from jax.sharding import Mesh
from jax.sharding import PartitionSpec as P

HOURS = 24
Z, X, CORES = (8, 4, 2)


TAU = 0.25
SIGMA_FLOW = 4.0
SIGMA_STORE = 0.25
KAPPA = 1.0
THETA = 0.5

AREAS = ("z", "x", "core")
CHIPS = ("z", "x")


def rounded(x):
    return lax.reduce_precision(x, 8, 7)


def swapped(x):
    return lax.ppermute(x, "core", [(0, 1), (1, 0)])


CONTRACT_MAJOR = (((0,), (0,)), ((), ()))
CONTRACT_MINOR = (((1,), (1,)), ((), ()))


def from_side(x, step):
    return lax.ppermute(x, "lines", [(i, i ^ step) for i in range(4)])


def with_side(x, step):
    other = from_side(x, step)
    return (x.astype(jnp.float32) + other.astype(jnp.float32)).astype(jnp.bfloat16)


def summed_pairs(halves):
    first, second = with_side(halves[0], 1), with_side(halves[1], 3)
    return first, from_side(first, 3), second, from_side(second, 1)


def store_price(dual_own, dual_other, weight_own, weight_other, first, second):
    price = lax.dot_general(
        dual_own[...], weight_own[...], CONTRACT_MAJOR, preferred_element_type=jnp.float32
    ) + lax.dot_general(
        dual_other[...], weight_other[...], CONTRACT_MAJOR, preferred_element_type=jnp.float32
    )
    rows = first.shape[0]
    first[...] = price[:rows].astype(jnp.bfloat16)
    second[...] = price[rows:].astype(jnp.bfloat16)


def weights_body(
    core,
    columns,
    column,
    stor_own,
    stor_other,
    dual_own,
    dual_other,
    weight_own,
    weight_other,
    first,
    second,
    split,
):
    slot_count, gen_count = columns.shape[0], column.shape[1]
    slot = lax.broadcasted_iota(jnp.int32, (slot_count, gen_count), 0)
    pick = jnp.where(slot == column[...], 1.0, 0.0).astype(jnp.bfloat16)
    weight = lax.dot_general(
        columns[...], pick, CONTRACT_MAJOR, preferred_element_type=jnp.float32
    )
    split[...] = weight.astype(jnp.bfloat16).reshape(split.shape)
    share_len = split.shape[1]
    mine = core[0]
    for chip in range(split.shape[0] // CORES):
        rows = slice(chip * share_len, (chip + 1) * share_len)
        weight_own[rows, :gen_count] = split[CORES * chip + mine]
        weight_other[rows, :gen_count] = split[CORES * chip + 1 - mine]
    weight_own[:, gen_count:] = stor_own[...]
    weight_other[:, gen_count:] = stor_other[...]
    store_price(dual_own, dual_other, weight_own, weight_other, first, second)


def price_body(dual_own, dual_other, weight_own, weight_other, first, second):
    store_price(dual_own, dual_other, weight_own, weight_other, first, second)


def in_fast(*arrays):
    return tuple(pltpu.with_memory_space_constraint(x, pltpu.VMEM) for x in arrays)


def half_prices(row_count, units):
    half = pltpu.VMEM((row_count // 2, units), jnp.bfloat16)
    return (half, half)


def weights_and_prices(core, columns, column, stor_own, stor_other, dual_own, dual_other):
    half_lines, row_count = dual_own.shape
    gen_count = column.shape[0]
    units = gen_count + stor_own.shape[1]
    weight = pltpu.VMEM((half_lines, units), jnp.bfloat16)
    in_vmem = pl.BlockSpec(memory_space=pltpu.VMEM)
    share_len = columns.shape[1] // (Z * X * CORES)
    own, other, first, second = pl.pallas_call(
        weights_body,
        out_shape=(weight, weight, *half_prices(row_count, units)),
        in_specs=[pl.BlockSpec(memory_space=pltpu.SMEM)] + [in_vmem] * 6,
        out_specs=(in_vmem,) * 4,
        scratch_shapes=[pltpu.VMEM((Z * X * CORES, share_len, gen_count), jnp.bfloat16)],
        name="weights",
    )(
        core.reshape(1),
        *in_fast(columns),
        column.reshape(1, -1),
        *in_fast(stor_own, stor_other, dual_own, dual_other),
    )
    return own, other, (first, second)


def later_prices(dual_own, dual_other, weight_own, weight_other):
    in_vmem = pl.BlockSpec(memory_space=pltpu.VMEM)
    return pl.pallas_call(
        price_body,
        out_shape=half_prices(dual_own.shape[1], weight_own.shape[1]),
        in_specs=[in_vmem] * 4,
        out_specs=(in_vmem,) * 2,
        name="prices",
    )(*in_fast(dual_own, dual_other, weight_own, weight_other))


def update_body(*refs):
    (
        first,
        first_far,
        second,
        second_far,
        level,
        gen_quad,
        gen_lin,
        gen_max,
        stor_quad,
        stor_rate,
        back,
        gen_now,
        stor_now,
        *old,
        bar_low,
        gen_next,
        stor_next,
        total,
    ) = refs
    row_count, gen_count = gen_now.shape
    half = row_count // 2
    bars = []
    for i, (near, far) in enumerate(((first, first_far), (second, second_far))):
        rows = slice(i * half, (i + 1) * half)
        price = near[...].astype(jnp.float32) + far[...].astype(jnp.float32)
        gen, stor = gen_now[rows], stor_now[rows]
        gen_mid, stor_mid = gen, stor
        if old:
            gen_mid = gen + THETA * (gen - old[0][rows])
            stor_mid = stor + THETA * (stor - old[1][rows])
        gen_grad = 2.0 * gen_quad[...] * gen_mid + gen_lin[...] + level[rows] + price[:, :gen_count]
        moved = jnp.clip(gen_mid - TAU * gen_grad, 0.0, gen_max[...])
        stor_grad = 2.0 * stor_quad[...] * stor_mid + level[rows] + price[:, gen_count:] + back[rows]
        rate = stor_rate[...]
        shifted = jnp.clip(stor_mid - TAU * stor_grad, -rate, rate)
        gen_next[rows] = moved
        stor_next[rows] = shifted
        bar = jnp.concatenate([2.0 * moved - gen, 2.0 * shifted - stor], axis=1)
        bar_low[rows] = bar.astype(jnp.bfloat16)
        bars.append(bar)
    total[...] = lax.dot_general(
        jnp.ones((8, bars[0].shape[1]), jnp.float32),
        jnp.concatenate(bars, axis=0),
        CONTRACT_MINOR,
        precision=lax.Precision.HIGHEST,
        preferred_element_type=jnp.float32,
    )


def updated(pairs, level, gen_params, stor_params, back, gen_now, stor_now, old):
    row_count, gen_count = gen_now.shape
    stor_count = stor_now.shape[1]
    operands = (
        *in_fast(*pairs, level[:, None]),
        *(value[None, :] for value in gen_params),
        *(value[None, :] for value in stor_params),
        *in_fast(back),
        gen_now,
        stor_now,
        *old,
    )
    in_vmem = pl.BlockSpec(memory_space=pltpu.VMEM)
    return pl.pallas_call(
        update_body,
        out_shape=(
            pltpu.VMEM((row_count, gen_count + stor_count), jnp.bfloat16),
            pltpu.VMEM((row_count, gen_count), jnp.float32),
            pltpu.VMEM((row_count, stor_count), jnp.float32),
            pltpu.VMEM((8, row_count), jnp.float32),
        ),
        in_specs=[in_vmem] * len(operands),
        out_specs=(in_vmem,) * 4,
        name="update",
    )(*operands)


def sent_to_chips(x):
    size = Z * X
    sent = jnp.broadcast_to(x[None], (size, *x.shape))
    return lax.all_to_all(sent, CHIPS, 0, 0, tiled=True)


def gathered_duals(share):
    own = sent_to_chips(share.astype(jnp.bfloat16)).reshape(-1, share.shape[1])
    return own, swapped(own)


def doubled(x, axis, size, step, dim):
    other = lax.ppermute(x, axis, [(i, i ^ step) for i in range(size)])
    first = (lax.axis_index(axis) // step) % 2 == 0
    return jnp.where(
        first, jnp.concatenate([x, other], axis=dim), jnp.concatenate([other, x], axis=dim)
    )


def gathered_early(share):
    share_len, row_count = share.shape
    held = share.astype(jnp.bfloat16).reshape(1, 1, share_len, row_count)
    for step in (1, 2, 4):
        held = doubled(held, "z", Z, step, 0)
    near = [held]
    for step in (1, 2, 3):
        near.append(lax.ppermute(held, "x", [(i, i ^ step) for i in range(X)]))
    index = lax.axis_index("x")
    low, high = index % 2 == 0, index // 2 == 0

    def pair(first, second):
        return jnp.where(
            low,
            jnp.concatenate([first, second], axis=1),
            jnp.concatenate([second, first], axis=1),
        )

    mine, far = pair(near[0], near[1]), pair(near[2], near[3])
    held = jnp.where(
        high, jnp.concatenate([mine, far], axis=1), jnp.concatenate([far, mine], axis=1)
    )
    own = held.reshape(-1, row_count)
    return own, swapped(own)


def hour_sums(row_count, later):
    row = jnp.arange(row_count, dtype=jnp.int32)
    same = (row[:, None] // HOURS) == (row[None, :] // HOURS)
    side = (row[None, :] >= row[:, None]) if later else (row[None, :] <= row[:, None])
    return jnp.where(same & side, 1.0, 0.0).astype(jnp.float32)


def summed_hours(values, later):
    return jnp.dot(
        hour_sums(values.shape[0], later),
        values,
        precision=lax.Precision.HIGHEST,
        preferred_element_type=jnp.float32,
    )


def dual_step(dual_now, image_term, step_size, low_bound, high_bound):
    shifted = dual_now + step_size * image_term
    return shifted - step_size * jnp.clip(shifted / step_size, low_bound, high_bound)


def shards(
    ptdf,
    load,
    ratings,
    line_index,
    gen_bus,
    gen_quad,
    gen_lin,
    gen_max,
    gen_start,
    stor_bus,
    stor_quad,
    stor_rate,
    stor_energy,
    stor_start,
    lam_start,
    mu_start,
    omega_start,
):
    row_count = load.shape[0]
    line_count, bus_count = ptdf.shape
    gen_count = gen_bus.shape[0]
    stor_count = stor_bus.shape[0]
    area_count = Z * X * CORES
    chip_count = Z * X
    slots = max(8, (gen_count + area_count - 1) // area_count)
    share_len = line_count // area_count
    core = lax.axis_index("core")
    area = (lax.axis_index("z") * X + lax.axis_index("x")) * CORES + core

    target = gen_bus // bus_count
    local_bus = gen_bus % bus_count
    order = jnp.arange(gen_count, dtype=jnp.int32)
    earlier = (target[:, None] == target[None, :]) & (order[None, :] < order[:, None])
    column = target * slots + jnp.sum(earlier.astype(jnp.int32), axis=1)
    slot_of = jnp.arange(area_count * slots, dtype=jnp.int32)
    placed = slot_of[:, None] == column[None, :]
    slot_bus = jnp.sum(jnp.where(placed, local_bus[None, :] + 1, 0), axis=1) - 1
    wanted = lax.all_to_all(slot_bus.reshape(area_count, slots), AREAS, 0, 0, tiled=True)

    dual_flow = mu_start.T
    dual_own, dual_other = gathered_early(dual_flow)

    bus_ids = jnp.arange(bus_count, dtype=jnp.int32)
    sel_gen = (wanted.reshape(-1)[:, None] == bus_ids[None, :]).astype(jnp.bfloat16)
    sel_stor = (stor_bus[:, None] == bus_ids[None, :]).astype(jnp.bfloat16)
    sent_columns = lax.dot_general(
        sel_gen, ptdf, CONTRACT_MINOR, preferred_element_type=jnp.float32
    ).astype(jnp.bfloat16)
    columns = lax.all_to_all(sent_columns, AREAS, 0, 0, tiled=True)
    weight_stor = lax.dot_general(
        ptdf, sel_stor, CONTRACT_MINOR, preferred_element_type=jnp.float32
    ).astype(jnp.bfloat16)

    def by_core(x):
        split = x.reshape(chip_count, CORES, share_len, x.shape[1])
        own = lax.dynamic_index_in_dim(split, core, 1, keepdims=False)
        other = lax.dynamic_index_in_dim(split, 1 - core, 1, keepdims=False)
        return own.reshape(-1, x.shape[1]), other.reshape(-1, x.shape[1])

    weight_own, weight_other, halves = weights_and_prices(
        core,
        columns.reshape(-1, line_count),
        column,
        *by_core(weight_stor),
        dual_own,
        dual_other,
    )
    load_part = lax.dot_general(
        ptdf, load.astype(jnp.bfloat16), CONTRACT_MINOR, preferred_element_type=jnp.float32
    )
    load_own, load_other = by_core(load_part)
    load_flow = load_own + swapped(load_other)
    load_total = jnp.sum(load, axis=1)

    limit = jnp.take(ratings, lax.dynamic_slice_in_dim(line_index, area * share_len, share_len))[:, None]
    hour_of = jnp.arange(row_count, dtype=jnp.int32) % HOURS
    last_hour = (hour_of == HOURS - 1)[:, None]
    half_energy = (0.5 * stor_energy)[None, :]
    low_bound = jnp.where(last_hour, jnp.zeros_like(half_energy), -half_energy)
    high_bound = jnp.where(last_hour, jnp.zeros_like(half_energy), half_energy)
    total_units = (gen_count + stor_count) * area_count
    gen_now, stor_now = (gen_start, stor_start)
    gen_old, stor_old = (gen_start, stor_start)
    price_level, dual_store = (lam_start, omega_start)
    for iteration in range(2):
        if iteration > 0:
            halves = later_prices(dual_own, dual_other, weight_own, weight_other)
        back = summed_hours(dual_store, True)
        bar_low, gen_next, stor_next, total = updated(
            summed_pairs(halves),
            price_level,
            (gen_quad, gen_lin, gen_max),
            (stor_quad, stor_rate),
            back,
            gen_now,
            stor_now,
            (gen_old, stor_old) if iteration > 0 else (),
        )
        balance = total[0] - load_total
        stor_bar = 2.0 * stor_next - stor_now
        flow_other = lax.dot_general(
            weight_other, bar_low, CONTRACT_MINOR, preferred_element_type=jnp.float32
        )
        flow_own = lax.dot_general(
            weight_own, bar_low, CONTRACT_MINOR, preferred_element_type=jnp.float32
        )
        flow_part = flow_own + swapped(flow_other) - load_flow
        balance = balance + swapped(balance)
        high = rounded(balance)
        lanes = 128
        strips = row_count // lanes
        tail = jnp.concatenate(
            [
                high.reshape(strips, lanes),
                (balance - high).reshape(strips, lanes),
                jnp.zeros((8 - 2 * strips, lanes), jnp.float32),
            ],
            axis=0,
        )
        body = flow_part.reshape(chip_count, share_len, row_count)
        sent = jnp.concatenate(
            [body[:, :, i * lanes : (i + 1) * lanes] for i in range(strips)]
            + [jnp.broadcast_to(tail[None], (chip_count, 8, lanes))],
            axis=1,
        ).astype(jnp.bfloat16)
        received = lax.all_to_all(sent, CHIPS, 0, 0, tiled=True)
        summed = jnp.sum(received.astype(jnp.float32), axis=0)
        flow_share = jnp.concatenate(
            [summed[i * share_len : (i + 1) * share_len] for i in range(strips)], axis=1
        )
        tail = summed[strips * share_len :]
        balance = (tail[:strips] + tail[strips : 2 * strips]).reshape(row_count)
        dual_flow = dual_step(dual_flow, flow_share, SIGMA_FLOW, -limit, limit)
        if iteration == 0:
            dual_own, dual_other = gathered_duals(dual_flow)
        price_level = price_level + KAPPA / total_units * balance
        dual_store = dual_step(
            dual_store, summed_hours(stor_bar, False), SIGMA_STORE, low_bound, high_bound
        )
        gen_old, stor_old = (gen_now, stor_now)
        gen_now, stor_now = (gen_next, stor_next)
    return (gen_now, stor_now, price_level, dual_flow.T, dual_store)


def solution(mesh):
    fine = Mesh(
        mesh.devices.reshape(mesh.shape["lines"], Z, X, CORES), ("lines", "z", "x", "core")
    )
    by_area = P(AREAS)
    by_column = P(None, AREAS)
    return jax.shard_map(
        shards,
        mesh=fine,
        in_specs=(
            P("lines", AREAS),
            by_column,
            P(),
            P("lines"),
            by_area,
            by_area,
            by_area,
            by_area,
            by_column,
            by_area,
            by_area,
            by_area,
            by_area,
            by_column,
            P(),
            P(None, ("lines", *AREAS)),
            by_column,
        ),
        out_specs=(by_column, by_column, P(), P(None, ("lines", *AREAS)), by_column),
        check_vma=False,
    )
```

```python
import jax
import jax.numpy as jnp
from jax import lax
from jax.experimental import pallas as pl
from jax.experimental.pallas import tpu as pltpu
from jax.sharding import Mesh
from jax.sharding import PartitionSpec as P

HOURS = 24
Z, X, CORES = (8, 4, 2)


TAU = 0.25
SIGMA_FLOW = 4.0
SIGMA_STORE = 0.25
KAPPA = 1.0
THETA = 0.5

VMEM_LIMIT = 16 * 1024 * 1024
AREAS = ("z", "x", "core")
CHIPS = ("z", "x")


def rounded(x):
    return lax.reduce_precision(x, 8, 7)


def swapped(x):
    return lax.ppermute(x, "core", [(0, 1), (1, 0)])


CONTRACT_MAJOR = (((0,), (0,)), ((), ()))
CONTRACT_MINOR = (((1,), (1,)), ((), ()))


def from_side(x, step):
    return lax.ppermute(x, "lines", [(i, i ^ step) for i in range(4)])


def with_side(x, step):
    other = from_side(x, step)
    return (x.astype(jnp.float32) + other.astype(jnp.float32)).astype(jnp.bfloat16)


def summed_pairs(halves):
    first, second = with_side(halves[0], 1), with_side(halves[1], 3)
    return first, from_side(first, 3), second, from_side(second, 1)


def store_price(dual_own, dual_other, weight_own, weight_other, first, second):
    price = lax.dot_general(
        dual_own[...], weight_own[...], CONTRACT_MAJOR, preferred_element_type=jnp.float32
    ) + lax.dot_general(
        dual_other[...], weight_other[...], CONTRACT_MAJOR, preferred_element_type=jnp.float32
    )
    rows = first.shape[0]
    first[...] = price[:rows].astype(jnp.bfloat16)
    second[...] = price[rows:].astype(jnp.bfloat16)


def weights_body(
    core,
    columns,
    column,
    stor_own,
    stor_other,
    dual_own,
    dual_other,
    weight_own,
    weight_other,
    first,
    second,
    split,
):
    slot_count, gen_count = columns.shape[0], column.shape[1]
    slot = lax.broadcasted_iota(jnp.int32, (slot_count, gen_count), 0)
    pick = jnp.where(slot == column[...], 1.0, 0.0).astype(jnp.bfloat16)
    weight = lax.dot_general(
        columns[...], pick, CONTRACT_MAJOR, preferred_element_type=jnp.float32
    )
    split[...] = weight.astype(jnp.bfloat16).reshape(split.shape)
    share_len = split.shape[1]
    mine = core[0]
    for chip in range(split.shape[0] // CORES):
        rows = slice(chip * share_len, (chip + 1) * share_len)
        weight_own[rows, :gen_count] = split[CORES * chip + mine]
        weight_other[rows, :gen_count] = split[CORES * chip + 1 - mine]
    weight_own[:, gen_count:] = stor_own[...]
    weight_other[:, gen_count:] = stor_other[...]
    store_price(dual_own, dual_other, weight_own, weight_other, first, second)


def price_body(dual_own, dual_other, weight_own, weight_other, first, second):
    store_price(dual_own, dual_other, weight_own, weight_other, first, second)


def in_fast(*arrays):
    return tuple(pltpu.with_memory_space_constraint(x, pltpu.VMEM) for x in arrays)


def in_main(*arrays):
    return tuple(pltpu.with_memory_space_constraint(x, pltpu.HBM) for x in arrays)


def half_prices(row_count, units):
    half = pltpu.VMEM((row_count // 2, units), jnp.bfloat16)
    return (half, half)


def weights_and_prices(core, columns, column, stor_own, stor_other, dual_own, dual_other):
    half_lines, row_count = dual_own.shape
    gen_count = column.shape[0]
    units = gen_count + stor_own.shape[1]
    weight = pltpu.VMEM((half_lines, units), jnp.bfloat16)
    in_vmem = pl.BlockSpec(memory_space=pltpu.VMEM)
    share_len = columns.shape[1] // (Z * X * CORES)
    own, other, first, second = pl.pallas_call(
        weights_body,
        out_shape=(weight, weight, *half_prices(row_count, units)),
        in_specs=[pl.BlockSpec(memory_space=pltpu.SMEM)] + [in_vmem] * 6,
        out_specs=(in_vmem,) * 4,
        scratch_shapes=[pltpu.VMEM((Z * X * CORES, share_len, gen_count), jnp.bfloat16)],
        name="weights",
        compiler_params=pltpu.CompilerParams(vmem_limit_bytes=VMEM_LIMIT),
    )(
        core.reshape(1),
        *in_fast(columns),
        column.reshape(1, -1),
        *in_fast(stor_own, stor_other, dual_own, dual_other),
    )
    return own, other, (first, second)


def later_prices(dual_own, dual_other, weight_own, weight_other):
    in_vmem = pl.BlockSpec(memory_space=pltpu.VMEM)
    return pl.pallas_call(
        price_body,
        out_shape=half_prices(dual_own.shape[1], weight_own.shape[1]),
        in_specs=[in_vmem] * 4,
        out_specs=(in_vmem,) * 2,
        name="prices",
        compiler_params=pltpu.CompilerParams(vmem_limit_bytes=VMEM_LIMIT),
    )(*in_fast(dual_own, dual_other, weight_own, weight_other))


def update_body(*refs):
    (
        first,
        first_far,
        second,
        second_far,
        level,
        gen_quad,
        gen_lin,
        gen_max,
        stor_quad,
        stor_rate,
        back,
        gen_now,
        stor_now,
        *old,
        bar_low,
        gen_next,
        stor_next,
        total,
    ) = refs
    row_count, gen_count = gen_now.shape
    half = row_count // 2
    bars = []
    for i, (near, far) in enumerate(((first, first_far), (second, second_far))):
        rows = slice(i * half, (i + 1) * half)
        price = near[...].astype(jnp.float32) + far[...].astype(jnp.float32)
        gen, stor = gen_now[rows], stor_now[rows]
        gen_mid, stor_mid = gen, stor
        if old:
            gen_mid = gen + THETA * (gen - old[0][rows])
            stor_mid = stor + THETA * (stor - old[1][rows])
        gen_grad = 2.0 * gen_quad[...] * gen_mid + gen_lin[...] + level[rows] + price[:, :gen_count]
        moved = jnp.clip(gen_mid - TAU * gen_grad, 0.0, gen_max[...])
        stor_grad = 2.0 * stor_quad[...] * stor_mid + level[rows] + price[:, gen_count:] + back[rows]
        rate = stor_rate[...]
        shifted = jnp.clip(stor_mid - TAU * stor_grad, -rate, rate)
        gen_next[rows] = moved
        stor_next[rows] = shifted
        bar = jnp.concatenate([2.0 * moved - gen, 2.0 * shifted - stor], axis=1)
        bar_low[rows] = bar.astype(jnp.bfloat16)
        bars.append(bar)
    total[...] = lax.dot_general(
        jnp.ones((8, bars[0].shape[1]), jnp.float32),
        jnp.concatenate(bars, axis=0),
        CONTRACT_MINOR,
        precision=lax.Precision.HIGHEST,
        preferred_element_type=jnp.float32,
    )


def updated(pairs, level, gen_params, stor_params, back, gen_now, stor_now, old):
    row_count, gen_count = gen_now.shape
    stor_count = stor_now.shape[1]
    operands = (
        *in_fast(*pairs, level[:, None]),
        *in_main(
            *(value[None, :] for value in gen_params),
            *(value[None, :] for value in stor_params),
            back,
            gen_now,
            stor_now,
            *old,
        ),
    )
    in_vmem = pl.BlockSpec(memory_space=pltpu.VMEM)
    return pl.pallas_call(
        update_body,
        out_shape=(
            pltpu.VMEM((row_count, gen_count + stor_count), jnp.bfloat16),
            pltpu.VMEM((row_count, gen_count), jnp.float32),
            pltpu.VMEM((row_count, stor_count), jnp.float32),
            pltpu.VMEM((8, row_count), jnp.float32),
        ),
        in_specs=[in_vmem] * len(operands),
        out_specs=(in_vmem,) * 4,
        name="update",
        compiler_params=pltpu.CompilerParams(vmem_limit_bytes=VMEM_LIMIT),
    )(*operands)


def sent_to_chips(x):
    size = Z * X
    sent = jnp.broadcast_to(x[None], (size, *x.shape))
    return lax.all_to_all(sent, CHIPS, 0, 0, tiled=True)


def gathered_duals(share):
    own = sent_to_chips(share.astype(jnp.bfloat16)).reshape(-1, share.shape[1])
    return own, swapped(own)


def doubled(x, axis, size, step, dim):
    other = lax.ppermute(x, axis, [(i, i ^ step) for i in range(size)])
    first = (lax.axis_index(axis) // step) % 2 == 0
    return jnp.where(
        first, jnp.concatenate([x, other], axis=dim), jnp.concatenate([other, x], axis=dim)
    )


def gathered_early(share):
    share_len, row_count = share.shape
    held = share.astype(jnp.bfloat16).reshape(1, 1, 1, share_len, row_count)
    for dim, step in enumerate((4, 2, 1)):
        held = doubled(held, "z", Z, step, dim)
    held = held.reshape(Z, 1, share_len, row_count)
    near = [held]
    for step in (1, 2, 3):
        near.append(lax.ppermute(held, "x", [(i, i ^ step) for i in range(X)]))
    index = lax.axis_index("x")
    low, high = index % 2 == 0, index // 2 == 0

    def pair(first, second):
        return jnp.where(
            low,
            jnp.concatenate([first, second], axis=1),
            jnp.concatenate([second, first], axis=1),
        )

    mine, far = pair(near[0], near[1]), pair(near[2], near[3])
    held = jnp.where(
        high, jnp.concatenate([mine, far], axis=1), jnp.concatenate([far, mine], axis=1)
    )
    own = held.reshape(-1, row_count)
    return own, swapped(own)


def hour_sums(row_count, later):
    row = jnp.arange(row_count, dtype=jnp.int32)
    same = (row[:, None] // HOURS) == (row[None, :] // HOURS)
    side = (row[None, :] >= row[:, None]) if later else (row[None, :] <= row[:, None])
    return jnp.where(same & side, 1.0, 0.0).astype(jnp.float32)


def summed_hours(values, later):
    return jnp.dot(
        hour_sums(values.shape[0], later),
        values,
        precision=lax.Precision.HIGHEST,
        preferred_element_type=jnp.float32,
    )


def dual_step(dual_now, image_term, step_size, low_bound, high_bound):
    shifted = dual_now + step_size * image_term
    return shifted - step_size * jnp.clip(shifted / step_size, low_bound, high_bound)


def shards(
    ptdf,
    load,
    ratings,
    line_index,
    gen_bus,
    gen_quad,
    gen_lin,
    gen_max,
    gen_start,
    stor_bus,
    stor_quad,
    stor_rate,
    stor_energy,
    stor_start,
    lam_start,
    mu_start,
    omega_start,
):
    row_count = load.shape[0]
    line_count, bus_count = ptdf.shape
    gen_count = gen_bus.shape[0]
    stor_count = stor_bus.shape[0]
    area_count = Z * X * CORES
    chip_count = Z * X
    slots = max(8, (gen_count + area_count - 1) // area_count)
    share_len = line_count // area_count
    core = lax.axis_index("core")
    area = (lax.axis_index("z") * X + lax.axis_index("x")) * CORES + core

    target = gen_bus // bus_count
    local_bus = gen_bus % bus_count
    order = jnp.arange(gen_count, dtype=jnp.int32)
    earlier = (target[:, None] == target[None, :]) & (order[None, :] < order[:, None])
    column = target * slots + jnp.sum(earlier.astype(jnp.int32), axis=1)
    slot_of = jnp.arange(area_count * slots, dtype=jnp.int32)
    placed = slot_of[:, None] == column[None, :]
    slot_bus = jnp.sum(jnp.where(placed, local_bus[None, :] + 1, 0), axis=1) - 1
    wanted = lax.all_to_all(slot_bus.reshape(area_count, slots), AREAS, 0, 0, tiled=True)

    dual_flow = mu_start.T
    dual_own, dual_other = gathered_early(dual_flow)

    bus_ids = jnp.arange(bus_count, dtype=jnp.int32)
    sel_gen = (wanted.reshape(-1)[:, None] == bus_ids[None, :]).astype(jnp.bfloat16)
    sel_stor = (stor_bus[:, None] == bus_ids[None, :]).astype(jnp.bfloat16)
    sent_columns = lax.dot_general(
        sel_gen, ptdf, CONTRACT_MINOR, preferred_element_type=jnp.float32
    ).astype(jnp.bfloat16)
    columns = lax.all_to_all(sent_columns, AREAS, 0, 0, tiled=True)
    weight_stor = lax.dot_general(
        ptdf, sel_stor, CONTRACT_MINOR, preferred_element_type=jnp.float32
    ).astype(jnp.bfloat16)

    def by_core(x):
        split = x.reshape(chip_count, CORES, share_len, x.shape[1])
        own = lax.dynamic_index_in_dim(split, core, 1, keepdims=False)
        other = lax.dynamic_index_in_dim(split, 1 - core, 1, keepdims=False)
        return own.reshape(-1, x.shape[1]), other.reshape(-1, x.shape[1])

    weight_own, weight_other, halves = weights_and_prices(
        core,
        columns.reshape(-1, line_count),
        column,
        *by_core(weight_stor),
        dual_own,
        dual_other,
    )
    load_part = lax.dot_general(
        ptdf, load.astype(jnp.bfloat16), CONTRACT_MINOR, preferred_element_type=jnp.float32
    )
    load_own, load_other = by_core(load_part)
    load_flow = load_own + swapped(load_other)
    load_total = jnp.sum(load, axis=1)

    weight_far = swapped(weight_other)
    limit = jnp.take(ratings, lax.dynamic_slice_in_dim(line_index, area * share_len, share_len))[:, None]
    hour_of = jnp.arange(row_count, dtype=jnp.int32) % HOURS
    last_hour = (hour_of == HOURS - 1)[:, None]
    half_energy = (0.5 * stor_energy)[None, :]
    low_bound = jnp.where(last_hour, jnp.zeros_like(half_energy), -half_energy)
    high_bound = jnp.where(last_hour, jnp.zeros_like(half_energy), half_energy)
    total_units = (gen_count + stor_count) * area_count
    gen_now, stor_now = (gen_start, stor_start)
    gen_old, stor_old = (gen_start, stor_start)
    price_level, dual_store = (lam_start, omega_start)
    for iteration in range(2):
        if iteration > 0:
            halves = later_prices(dual_own, dual_other, weight_own, weight_other)
        back = summed_hours(dual_store, True)
        bar_low, gen_next, stor_next, total = updated(
            summed_pairs(halves),
            price_level,
            (gen_quad, gen_lin, gen_max),
            (stor_quad, stor_rate),
            back,
            gen_now,
            stor_now,
            (gen_old, stor_old) if iteration > 0 else (),
        )
        balance = total[0] - load_total
        stor_bar = 2.0 * stor_next - stor_now
        flow_part = (
            lax.dot_general(weight_own, bar_low, CONTRACT_MINOR, preferred_element_type=jnp.float32)
            + lax.dot_general(
                weight_far, swapped(bar_low), CONTRACT_MINOR, preferred_element_type=jnp.float32
            )
            - load_flow
        )
        balance = balance + swapped(balance)
        high = rounded(balance)
        lanes = 128
        strips = row_count // lanes
        tail = jnp.concatenate(
            [
                high.reshape(strips, lanes),
                (balance - high).reshape(strips, lanes),
                jnp.zeros((8 - 2 * strips, lanes), jnp.float32),
            ],
            axis=0,
        )
        body = flow_part.reshape(chip_count, share_len, row_count)
        sent = jnp.concatenate(
            [body[:, :, i * lanes : (i + 1) * lanes] for i in range(strips)]
            + [jnp.broadcast_to(tail[None], (chip_count, 8, lanes))],
            axis=1,
        ).astype(jnp.bfloat16)
        received = lax.all_to_all(sent, CHIPS, 0, 0, tiled=True)
        summed = jnp.sum(received.astype(jnp.float32), axis=0)
        flow_share = jnp.concatenate(
            [summed[i * share_len : (i + 1) * share_len] for i in range(strips)], axis=1
        )
        tail = summed[strips * share_len :]
        balance = (tail[:strips] + tail[strips : 2 * strips]).reshape(row_count)
        dual_flow = dual_step(dual_flow, flow_share, SIGMA_FLOW, -limit, limit)
        if iteration == 0:
            dual_own, dual_other = gathered_duals(dual_flow)
        price_level = price_level + KAPPA / total_units * balance
        dual_store = dual_step(
            dual_store, summed_hours(stor_bar, False), SIGMA_STORE, low_bound, high_bound
        )
        gen_old, stor_old = (gen_now, stor_now)
        gen_now, stor_now = (gen_next, stor_next)
    return (gen_now, stor_now, price_level, dual_flow.T, dual_store)


def solution(mesh):
    fine = Mesh(
        mesh.devices.reshape(mesh.shape["lines"], Z, X, CORES), ("lines", "z", "x", "core")
    )
    by_area = P(AREAS)
    by_column = P(None, AREAS)
    return jax.shard_map(
        shards,
        mesh=fine,
        in_specs=(
            P("lines", AREAS),
            by_column,
            P(),
            P("lines"),
            by_area,
            by_area,
            by_area,
            by_area,
            by_column,
            by_area,
            by_area,
            by_area,
            by_area,
            by_column,
            P(),
            P(None, ("lines", *AREAS)),
            by_column,
        ),
        out_specs=(by_column, by_column, P(), P(None, ("lines", *AREAS)), by_column),
        check_vma=False,
    )
```

```python
import jax
import jax.numpy as jnp
from jax import lax
from jax.experimental import pallas as pl
from jax.experimental.pallas import tpu as pltpu
from jax.sharding import Mesh
from jax.sharding import PartitionSpec as P

HOURS = 24
Z, X, CORES = (8, 4, 2)


TAU = 0.25
SIGMA_FLOW = 4.0
SIGMA_STORE = 0.25
KAPPA = 1.0
THETA = 0.5

VMEM_LIMIT = 16 * 1024 * 1024
AREAS = ("z", "x", "core")
CHIPS = ("z", "x")


def rounded(x):
    return lax.reduce_precision(x, 8, 7)


def swapped(x):
    return lax.ppermute(x, "core", [(0, 1), (1, 0)])


CONTRACT_MAJOR = (((0,), (0,)), ((), ()))
CONTRACT_MINOR = (((1,), (1,)), ((), ()))


def from_side(x, step):
    return lax.ppermute(x, "lines", [(i, i ^ step) for i in range(4)])


def with_side(x, step):
    other = from_side(x, step)
    return (x.astype(jnp.float32) + other.astype(jnp.float32)).astype(jnp.bfloat16)


def summed_pairs(halves):
    first, second = with_side(halves[0], 1), with_side(halves[1], 3)
    return first, from_side(first, 3), second, from_side(second, 1)


def store_price(dual_own, dual_other, weight_own, weight_other, first, second):
    price = lax.dot_general(
        dual_own[...], weight_own[...], CONTRACT_MAJOR, preferred_element_type=jnp.float32
    ) + lax.dot_general(
        dual_other[...], weight_other[...], CONTRACT_MAJOR, preferred_element_type=jnp.float32
    )
    rows = first.shape[0]
    first[...] = price[:rows].astype(jnp.bfloat16)
    second[...] = price[rows:].astype(jnp.bfloat16)


def weights_body(
    core,
    columns,
    column,
    stor_own,
    stor_other,
    dual_own,
    dual_other,
    weight_own,
    weight_other,
    first,
    second,
    split,
):
    slot_count, gen_count = columns.shape[0], column.shape[1]
    slot = lax.broadcasted_iota(jnp.int32, (slot_count, gen_count), 0)
    pick = jnp.where(slot == column[...], 1.0, 0.0).astype(jnp.bfloat16)
    weight = lax.dot_general(
        columns[...], pick, CONTRACT_MAJOR, preferred_element_type=jnp.float32
    )
    split[...] = weight.astype(jnp.bfloat16).reshape(split.shape)
    share_len = split.shape[1]
    mine = core[0]
    for chip in range(split.shape[0] // CORES):
        rows = slice(chip * share_len, (chip + 1) * share_len)
        weight_own[rows, :gen_count] = split[CORES * chip + mine]
        weight_other[rows, :gen_count] = split[CORES * chip + 1 - mine]
    weight_own[:, gen_count:] = stor_own[...]
    weight_other[:, gen_count:] = stor_other[...]
    store_price(dual_own, dual_other, weight_own, weight_other, first, second)


def price_body(dual_own, dual_other, weight_own, weight_other, first, second):
    store_price(dual_own, dual_other, weight_own, weight_other, first, second)


def in_fast(*arrays):
    return tuple(pltpu.with_memory_space_constraint(x, pltpu.VMEM) for x in arrays)


def in_main(*arrays):
    return tuple(pltpu.with_memory_space_constraint(x, pltpu.HBM) for x in arrays)


def half_prices(row_count, units):
    half = pltpu.VMEM((row_count // 2, units), jnp.bfloat16)
    return (half, half)


def weights_and_prices(core, columns, column, stor_own, stor_other, dual_own, dual_other):
    half_lines, row_count = dual_own.shape
    gen_count = column.shape[0]
    units = gen_count + stor_own.shape[1]
    weight = pltpu.VMEM((half_lines, units), jnp.bfloat16)
    in_vmem = pl.BlockSpec(memory_space=pltpu.VMEM)
    share_len = columns.shape[1] // (Z * X * CORES)
    own, other, first, second = pl.pallas_call(
        weights_body,
        out_shape=(weight, weight, *half_prices(row_count, units)),
        in_specs=[pl.BlockSpec(memory_space=pltpu.SMEM)] + [in_vmem] * 6,
        out_specs=(in_vmem,) * 4,
        scratch_shapes=[pltpu.VMEM((Z * X * CORES, share_len, gen_count), jnp.bfloat16)],
        name="weights",
        compiler_params=pltpu.CompilerParams(vmem_limit_bytes=VMEM_LIMIT),
    )(
        core.reshape(1),
        *in_fast(columns),
        column.reshape(1, -1),
        *in_main(stor_own, stor_other, dual_own, dual_other),
    )
    return own, other, (first, second)


def later_prices(dual_own, dual_other, weight_own, weight_other):
    in_vmem = pl.BlockSpec(memory_space=pltpu.VMEM)
    return pl.pallas_call(
        price_body,
        out_shape=half_prices(dual_own.shape[1], weight_own.shape[1]),
        in_specs=[in_vmem] * 4,
        out_specs=(in_vmem,) * 2,
        name="prices",
        compiler_params=pltpu.CompilerParams(vmem_limit_bytes=VMEM_LIMIT),
    )(*in_fast(dual_own, dual_other), *in_main(weight_own, weight_other))


def dual_body(received, dual, limit, tail, dual_next, *sent):
    total = jnp.sum(received[...].astype(jnp.float32), axis=0)
    share_len = dual.shape[0]
    strips = dual.shape[1] // total.shape[1]
    flow = jnp.concatenate(
        [total[i * share_len : (i + 1) * share_len] for i in range(strips)], axis=1
    )
    tail[...] = total[strips * share_len :]
    bound = limit[...]
    moved = dual_step(dual[...], flow, SIGMA_FLOW, -bound, bound)
    dual_next[...] = moved
    for out in sent:
        out[...] = jnp.broadcast_to(moved.astype(jnp.bfloat16)[None], out.shape)


def dual_updated(received, dual, limit, spread):
    chips, _, lanes = received.shape
    in_vmem = pl.BlockSpec(memory_space=pltpu.VMEM)
    out_shape = (
        jax.ShapeDtypeStruct((8, lanes), jnp.float32),
        jax.ShapeDtypeStruct(dual.shape, jnp.float32),
    )
    if spread:
        out_shape += (pltpu.HBM((chips, *dual.shape), jnp.bfloat16),)
    return pl.pallas_call(
        dual_body,
        out_shape=out_shape,
        in_specs=[in_vmem] * 3,
        out_specs=(in_vmem,) * len(out_shape),
        name="duals",
        compiler_params=pltpu.CompilerParams(vmem_limit_bytes=VMEM_LIMIT),
    )(received, dual, limit)


def update_body(*refs):
    (
        first,
        first_far,
        second,
        second_far,
        level,
        gen_quad,
        gen_lin,
        gen_max,
        stor_quad,
        stor_rate,
        back,
        gen_now,
        stor_now,
        *old,
        bar_low,
        gen_next,
        stor_next,
        total,
    ) = refs
    row_count, gen_count = gen_now.shape
    half = row_count // 2
    bars = []
    for i, (near, far) in enumerate(((first, first_far), (second, second_far))):
        rows = slice(i * half, (i + 1) * half)
        price = near[...].astype(jnp.float32) + far[...].astype(jnp.float32)
        gen, stor = gen_now[rows], stor_now[rows]
        gen_mid, stor_mid = gen, stor
        if old:
            gen_mid = gen + THETA * (gen - old[0][rows])
            stor_mid = stor + THETA * (stor - old[1][rows])
        gen_grad = 2.0 * gen_quad[...] * gen_mid + gen_lin[...] + level[rows] + price[:, :gen_count]
        moved = jnp.clip(gen_mid - TAU * gen_grad, 0.0, gen_max[...])
        stor_grad = 2.0 * stor_quad[...] * stor_mid + level[rows] + price[:, gen_count:] + back[rows]
        rate = stor_rate[...]
        shifted = jnp.clip(stor_mid - TAU * stor_grad, -rate, rate)
        gen_next[rows] = moved
        stor_next[rows] = shifted
        bar = jnp.concatenate([2.0 * moved - gen, 2.0 * shifted - stor], axis=1)
        bar_low[rows] = bar.astype(jnp.bfloat16)
        bars.append(bar)
    total[...] = lax.dot_general(
        jnp.ones((8, bars[0].shape[1]), jnp.float32),
        jnp.concatenate(bars, axis=0),
        CONTRACT_MINOR,
        precision=lax.Precision.HIGHEST,
        preferred_element_type=jnp.float32,
    )


def updated(pairs, level, gen_params, stor_params, back, gen_now, stor_now, old):
    row_count, gen_count = gen_now.shape
    stor_count = stor_now.shape[1]
    operands = (
        *in_fast(*pairs, level[:, None]),
        *in_main(
            *(value[None, :] for value in gen_params),
            *(value[None, :] for value in stor_params),
            back,
            gen_now,
            stor_now,
            *old,
        ),
    )
    in_vmem = pl.BlockSpec(memory_space=pltpu.VMEM)
    return pl.pallas_call(
        update_body,
        out_shape=(
            pltpu.VMEM((row_count, gen_count + stor_count), jnp.bfloat16),
            pltpu.VMEM((row_count, gen_count), jnp.float32),
            pltpu.VMEM((row_count, stor_count), jnp.float32),
            pltpu.VMEM((8, row_count), jnp.float32),
        ),
        in_specs=[in_vmem] * len(operands),
        out_specs=(in_vmem,) * 4,
        name="update",
        compiler_params=pltpu.CompilerParams(vmem_limit_bytes=VMEM_LIMIT),
    )(*operands)


def gathered_duals(sent):
    own = lax.all_to_all(sent, CHIPS, 0, 0, tiled=True).reshape(-1, sent.shape[2])
    return own, swapped(own)


def doubled(x, axis, size, step, dim):
    other = lax.ppermute(x, axis, [(i, i ^ step) for i in range(size)])
    first = (lax.axis_index(axis) // step) % 2 == 0
    return jnp.where(
        first, jnp.concatenate([x, other], axis=dim), jnp.concatenate([other, x], axis=dim)
    )


def gathered_early(share):
    share_len, row_count = share.shape
    held = share.astype(jnp.bfloat16).reshape(1, 1, 1, share_len, row_count)
    for dim, step in enumerate((4, 2, 1)):
        held = doubled(held, "z", Z, step, dim)
    held = held.reshape(Z, 1, share_len, row_count)
    near = [held]
    for step in (1, 2, 3):
        near.append(lax.ppermute(held, "x", [(i, i ^ step) for i in range(X)]))
    index = lax.axis_index("x")
    low, high = index % 2 == 0, index // 2 == 0

    def pair(first, second):
        return jnp.where(
            low,
            jnp.concatenate([first, second], axis=1),
            jnp.concatenate([second, first], axis=1),
        )

    mine, far = pair(near[0], near[1]), pair(near[2], near[3])
    held = jnp.where(
        high, jnp.concatenate([mine, far], axis=1), jnp.concatenate([far, mine], axis=1)
    )
    own = held.reshape(-1, row_count)
    return own, swapped(own)


def hour_sums(row_count, later):
    row = jnp.arange(row_count, dtype=jnp.int32)
    same = (row[:, None] // HOURS) == (row[None, :] // HOURS)
    side = (row[None, :] >= row[:, None]) if later else (row[None, :] <= row[:, None])
    return jnp.where(same & side, 1.0, 0.0).astype(jnp.float32)


def summed_hours(values, later):
    return jnp.dot(
        hour_sums(values.shape[0], later),
        values,
        precision=lax.Precision.HIGHEST,
        preferred_element_type=jnp.float32,
    )


def dual_step(dual_now, image_term, step_size, low_bound, high_bound):
    shifted = dual_now + step_size * image_term
    return shifted - step_size * jnp.clip(shifted / step_size, low_bound, high_bound)


def shards(
    ptdf,
    load,
    ratings,
    line_index,
    gen_bus,
    gen_quad,
    gen_lin,
    gen_max,
    gen_start,
    stor_bus,
    stor_quad,
    stor_rate,
    stor_energy,
    stor_start,
    lam_start,
    mu_start,
    omega_start,
):
    row_count = load.shape[0]
    line_count, bus_count = ptdf.shape
    gen_count = gen_bus.shape[0]
    stor_count = stor_bus.shape[0]
    area_count = Z * X * CORES
    chip_count = Z * X
    slots = max(8, (gen_count + area_count - 1) // area_count)
    share_len = line_count // area_count
    core = lax.axis_index("core")
    area = (lax.axis_index("z") * X + lax.axis_index("x")) * CORES + core

    target = gen_bus // bus_count
    local_bus = gen_bus % bus_count
    order = jnp.arange(gen_count, dtype=jnp.int32)
    earlier = (target[:, None] == target[None, :]) & (order[None, :] < order[:, None])
    column = target * slots + jnp.sum(earlier.astype(jnp.int32), axis=1)
    slot_of = jnp.arange(area_count * slots, dtype=jnp.int32)
    placed = slot_of[:, None] == column[None, :]
    slot_bus = jnp.sum(jnp.where(placed, local_bus[None, :] + 1, 0), axis=1) - 1
    wanted = lax.all_to_all(slot_bus.reshape(area_count, slots), AREAS, 0, 0, tiled=True)

    dual_flow = mu_start.T
    dual_own, dual_other = gathered_early(dual_flow)

    bus_ids = jnp.arange(bus_count, dtype=jnp.int32)
    sel_gen = (wanted.reshape(-1)[:, None] == bus_ids[None, :]).astype(jnp.bfloat16)
    sel_stor = (stor_bus[:, None] == bus_ids[None, :]).astype(jnp.bfloat16)
    sent_columns = lax.dot_general(
        sel_gen, ptdf, CONTRACT_MINOR, preferred_element_type=jnp.float32
    ).astype(jnp.bfloat16)
    columns = lax.all_to_all(sent_columns, AREAS, 0, 0, tiled=True)
    weight_stor = lax.dot_general(
        ptdf, sel_stor, CONTRACT_MINOR, preferred_element_type=jnp.float32
    ).astype(jnp.bfloat16)

    def by_core(x):
        split = x.reshape(chip_count, CORES, share_len, x.shape[1])
        own = lax.dynamic_index_in_dim(split, core, 1, keepdims=False)
        other = lax.dynamic_index_in_dim(split, 1 - core, 1, keepdims=False)
        return own.reshape(-1, x.shape[1]), other.reshape(-1, x.shape[1])

    weight_own, weight_other, halves = weights_and_prices(
        core,
        columns.reshape(-1, line_count),
        column,
        *by_core(weight_stor),
        dual_own,
        dual_other,
    )
    load_part = lax.dot_general(
        ptdf, load.astype(jnp.bfloat16), CONTRACT_MINOR, preferred_element_type=jnp.float32
    )
    load_own, load_other = by_core(load_part)
    load_flow = load_own + swapped(load_other)
    load_total = jnp.sum(load, axis=1)

    weight_far = swapped(weight_other)
    limit = jnp.take(ratings, lax.dynamic_slice_in_dim(line_index, area * share_len, share_len))[:, None]
    hour_of = jnp.arange(row_count, dtype=jnp.int32) % HOURS
    last_hour = (hour_of == HOURS - 1)[:, None]
    half_energy = (0.5 * stor_energy)[None, :]
    low_bound = jnp.where(last_hour, jnp.zeros_like(half_energy), -half_energy)
    high_bound = jnp.where(last_hour, jnp.zeros_like(half_energy), half_energy)
    total_units = (gen_count + stor_count) * area_count
    gen_now, stor_now = (gen_start, stor_start)
    gen_old, stor_old = (gen_start, stor_start)
    price_level, dual_store = (lam_start, omega_start)
    for iteration in range(2):
        if iteration > 0:
            halves = later_prices(dual_own, dual_other, weight_own, weight_other)
        back = summed_hours(dual_store, True)
        bar_low, gen_next, stor_next, total = updated(
            summed_pairs(halves),
            price_level,
            (gen_quad, gen_lin, gen_max),
            (stor_quad, stor_rate),
            back,
            gen_now,
            stor_now,
            (gen_old, stor_old) if iteration > 0 else (),
        )
        balance = total[0] - load_total
        stor_bar = 2.0 * stor_next - stor_now
        flow_part = (
            lax.dot_general(weight_own, bar_low, CONTRACT_MINOR, preferred_element_type=jnp.float32)
            + lax.dot_general(
                weight_far, swapped(bar_low), CONTRACT_MINOR, preferred_element_type=jnp.float32
            )
            - load_flow
        )
        balance = balance + swapped(balance)
        high = rounded(balance)
        lanes = 128
        strips = row_count // lanes
        tail = jnp.concatenate(
            [
                high.reshape(strips, lanes),
                (balance - high).reshape(strips, lanes),
                jnp.zeros((8 - 2 * strips, lanes), jnp.float32),
            ],
            axis=0,
        )
        body = flow_part.reshape(chip_count, share_len, row_count)
        sent = jnp.concatenate(
            [body[:, :, i * lanes : (i + 1) * lanes] for i in range(strips)]
            + [jnp.broadcast_to(tail[None], (chip_count, 8, lanes))],
            axis=1,
        ).astype(jnp.bfloat16)
        received = lax.all_to_all(sent, CHIPS, 0, 0, tiled=True)
        tail, dual_flow, *spread = dual_updated(received, dual_flow, limit, iteration == 0)
        balance = (tail[:strips] + tail[strips : 2 * strips]).reshape(row_count)
        if iteration == 0:
            dual_own, dual_other = gathered_duals(spread[0])
        price_level = price_level + KAPPA / total_units * balance
        dual_store = dual_step(
            dual_store, summed_hours(stor_bar, False), SIGMA_STORE, low_bound, high_bound
        )
        gen_old, stor_old = (gen_now, stor_now)
        gen_now, stor_now = (gen_next, stor_next)
    return (gen_now, stor_now, price_level, dual_flow.T, dual_store)


def solution(mesh):
    fine = Mesh(
        mesh.devices.reshape(mesh.shape["lines"], Z, X, CORES), ("lines", "z", "x", "core")
    )
    by_area = P(AREAS)
    by_column = P(None, AREAS)
    return jax.shard_map(
        shards,
        mesh=fine,
        in_specs=(
            P("lines", AREAS),
            by_column,
            P(),
            P("lines"),
            by_area,
            by_area,
            by_area,
            by_area,
            by_column,
            by_area,
            by_area,
            by_area,
            by_area,
            by_column,
            P(),
            P(None, ("lines", *AREAS)),
            by_column,
        ),
        out_specs=(by_column, by_column, P(), P(None, ("lines", *AREAS)), by_column),
        check_vma=False,
    )
```

```python
import jax
import jax.numpy as jnp
from jax import lax
from jax.experimental import pallas as pl
from jax.experimental.pallas import tpu as pltpu
from jax.sharding import Mesh
from jax.sharding import PartitionSpec as P

HOURS = 24
Z, X, CORES = (8, 4, 2)


TAU = 0.25
SIGMA_FLOW = 4.0
SIGMA_STORE = 0.25
KAPPA = 1.0
THETA = 0.5

VMEM_LIMIT = 16 * 1024 * 1024
AREAS = ("z", "x", "core")
CHIPS = ("z", "x")


def rounded(x):
    return lax.reduce_precision(x, 8, 7)


def swapped(x):
    return lax.ppermute(x, "core", [(0, 1), (1, 0)])


CONTRACT_MAJOR = (((0,), (0,)), ((), ()))
CONTRACT_MINOR = (((1,), (1,)), ((), ()))


def from_side(x, step):
    return lax.ppermute(x, "lines", [(i, i ^ step) for i in range(4)])


def with_side(x, step):
    other = from_side(x, step)
    return (x.astype(jnp.float32) + other.astype(jnp.float32)).astype(jnp.bfloat16)


def summed_pairs(halves):
    first = with_side(halves[0], 1)
    second = with_side(halves[1], 3)
    return first, from_side(first, 3), second, from_side(second, 1)


def store_price(dual_own, dual_other, weight_own, weight_other, first, second):
    price = lax.dot_general(
        dual_own[...], weight_own[...], CONTRACT_MAJOR, preferred_element_type=jnp.float32
    ) + lax.dot_general(
        dual_other[...], weight_other[...], CONTRACT_MAJOR, preferred_element_type=jnp.float32
    )
    rows = first.shape[0]
    first[...] = price[:rows].astype(jnp.bfloat16)
    second[...] = price[rows:].astype(jnp.bfloat16)


def weights_body(
    core,
    columns,
    column,
    stor_own,
    stor_other,
    dual_own,
    dual_other,
    weight_own,
    weight_other,
    first,
    second,
    split,
):
    slot_count, gen_count = columns.shape[0], column.shape[1]
    slot = lax.broadcasted_iota(jnp.int32, (slot_count, gen_count), 0)
    pick = jnp.where(slot == column[...], 1.0, 0.0).astype(jnp.bfloat16)
    weight = lax.dot_general(
        columns[...], pick, CONTRACT_MAJOR, preferred_element_type=jnp.float32
    )
    split[...] = weight.astype(jnp.bfloat16).reshape(split.shape)
    share_len = split.shape[1]
    mine = core[0]
    for chip in range(split.shape[0] // CORES):
        rows = slice(chip * share_len, (chip + 1) * share_len)
        weight_own[rows, :gen_count] = split[CORES * chip + mine]
        weight_other[rows, :gen_count] = split[CORES * chip + 1 - mine]
    weight_own[:, gen_count:] = stor_own[...]
    weight_other[:, gen_count:] = stor_other[...]
    store_price(dual_own, dual_other, weight_own, weight_other, first, second)


def price_body(dual_own, dual_other, weight_own, weight_other, first, second):
    store_price(dual_own, dual_other, weight_own, weight_other, first, second)


def in_fast(*arrays):
    return tuple(pltpu.with_memory_space_constraint(x, pltpu.VMEM) for x in arrays)


def in_main(*arrays):
    return tuple(pltpu.with_memory_space_constraint(x, pltpu.HBM) for x in arrays)


def half_prices(row_count, units):
    half = pltpu.VMEM((row_count // 2, units), jnp.bfloat16)
    return (half, half)


def weights_and_prices(core, columns, column, stor_own, stor_other, dual_own, dual_other):
    half_lines, row_count = dual_own.shape
    gen_count = column.shape[0]
    units = gen_count + stor_own.shape[1]
    weight = pltpu.VMEM((half_lines, units), jnp.bfloat16)
    in_vmem = pl.BlockSpec(memory_space=pltpu.VMEM)
    share_len = columns.shape[1] // (Z * X * CORES)
    own, other, first, second = pl.pallas_call(
        weights_body,
        out_shape=(weight, weight, *half_prices(row_count, units)),
        in_specs=[pl.BlockSpec(memory_space=pltpu.SMEM)] + [in_vmem] * 6,
        out_specs=(in_vmem,) * 4,
        scratch_shapes=[pltpu.VMEM((Z * X * CORES, share_len, gen_count), jnp.bfloat16)],
        name="weights",
        compiler_params=pltpu.CompilerParams(vmem_limit_bytes=VMEM_LIMIT),
    )(
        core.reshape(1),
        *in_fast(columns),
        column.reshape(1, -1),
        *in_main(stor_own, stor_other, dual_own, dual_other),
    )
    return own, other, (first, second)


def later_prices(dual_own, dual_other, weight_own, weight_other):
    in_vmem = pl.BlockSpec(memory_space=pltpu.VMEM)
    return pl.pallas_call(
        price_body,
        out_shape=half_prices(dual_own.shape[1], weight_own.shape[1]),
        in_specs=[in_vmem] * 4,
        out_specs=(in_vmem,) * 2,
        name="prices",
        compiler_params=pltpu.CompilerParams(vmem_limit_bytes=VMEM_LIMIT),
    )(*in_fast(dual_own, dual_other), *in_main(weight_own, weight_other))


def dual_body(received, dual, limit, tail, dual_next, *sent):
    total = jnp.sum(received[...].astype(jnp.float32), axis=0)
    share_len = dual.shape[0]
    strips = dual.shape[1] // total.shape[1]
    flow = jnp.concatenate(
        [total[i * share_len : (i + 1) * share_len] for i in range(strips)], axis=1
    )
    tail[...] = total[strips * share_len :]
    bound = limit[...]
    moved = dual_step(dual[...], flow, SIGMA_FLOW, -bound, bound)
    dual_next[...] = moved
    for out in sent:
        out[...] = jnp.broadcast_to(moved.astype(jnp.bfloat16)[None], out.shape)


def dual_updated(received, dual, limit, spread):
    chips, _, lanes = received.shape
    in_vmem = pl.BlockSpec(memory_space=pltpu.VMEM)
    out_shape = (
        jax.ShapeDtypeStruct((8, lanes), jnp.float32),
        jax.ShapeDtypeStruct(dual.shape, jnp.float32),
    )
    if spread:
        out_shape += (pltpu.HBM((chips, *dual.shape), jnp.bfloat16),)
    return pl.pallas_call(
        dual_body,
        out_shape=out_shape,
        in_specs=[in_vmem] * 3,
        out_specs=(in_vmem,) * len(out_shape),
        name="duals",
        compiler_params=pltpu.CompilerParams(vmem_limit_bytes=VMEM_LIMIT),
    )(*in_fast(received), dual, limit)


def base_body(level, gen_quad, gen_lin, stor_quad, back, gen_now, stor_now, *refs):
    *old, gen_base, stor_base, gen_held, stor_held = refs
    gen, stor = gen_now[...], stor_now[...]
    gen_mid, stor_mid = gen, stor
    if old:
        gen_mid = gen + THETA * (gen - old[0][...])
        stor_mid = stor + THETA * (stor - old[1][...])
    gen_cost = 2.0 * gen_quad[...] * gen_mid + gen_lin[...] + level[...]
    stor_cost = 2.0 * stor_quad[...] * stor_mid + level[...] + back[...]
    gen_base[...] = gen_mid - TAU * gen_cost
    stor_base[...] = stor_mid - TAU * stor_cost
    gen_held[...] = gen
    stor_held[...] = stor


def update_body(
    first,
    first_far,
    second,
    second_far,
    gen_base,
    stor_base,
    gen_now,
    stor_now,
    gen_max,
    stor_rate,
    bar_low,
    gen_next,
    stor_next,
    total,
):
    row_count, gen_count = gen_now.shape
    half = row_count // 2
    rate = stor_rate[...]
    bars = []
    for i, (near, far) in enumerate(((first, first_far), (second, second_far))):
        rows = slice(i * half, (i + 1) * half)
        change = TAU * (near[...].astype(jnp.float32) + far[...].astype(jnp.float32))
        moved = jnp.clip(gen_base[rows] - change[:, :gen_count], 0.0, gen_max[...])
        shifted = jnp.clip(stor_base[rows] - change[:, gen_count:], -rate, rate)
        gen_next[rows] = moved
        stor_next[rows] = shifted
        bar = jnp.concatenate(
            [2.0 * moved - gen_now[rows], 2.0 * shifted - stor_now[rows]], axis=1
        )
        bar_low[rows] = bar.astype(jnp.bfloat16)
        bars.append(bar)
    total[...] = lax.dot_general(
        jnp.ones((8, bars[0].shape[1]), jnp.float32),
        jnp.concatenate(bars, axis=0),
        CONTRACT_MINOR,
        precision=lax.Precision.HIGHEST,
        preferred_element_type=jnp.float32,
    )


def bases(level, gen_quad, gen_lin, stor_quad, back, gen_now, stor_now, old):
    operands = (
        *in_fast(level[:, None]),
        *in_main(
            gen_quad[None, :],
            gen_lin[None, :],
            stor_quad[None, :],
            back,
            gen_now,
            stor_now,
            *old,
        ),
    )
    in_vmem = pl.BlockSpec(memory_space=pltpu.VMEM)
    gen, stor = pltpu.VMEM(gen_now.shape, jnp.float32), pltpu.VMEM(stor_now.shape, jnp.float32)
    return pl.pallas_call(
        base_body,
        out_shape=(gen, stor, gen, stor),
        in_specs=[in_vmem] * len(operands),
        out_specs=(in_vmem,) * 4,
        name="bases",
        compiler_params=pltpu.CompilerParams(vmem_limit_bytes=VMEM_LIMIT),
    )(*operands)


def updated(pairs, held, gen_max, stor_rate):
    row_count, gen_count = held[0].shape
    stor_count = held[1].shape[1]
    operands = (*in_fast(*pairs, *held), *in_main(gen_max[None, :], stor_rate[None, :]))
    in_vmem = pl.BlockSpec(memory_space=pltpu.VMEM)
    return pl.pallas_call(
        update_body,
        out_shape=(
            pltpu.VMEM((row_count, gen_count + stor_count), jnp.bfloat16),
            pltpu.VMEM((row_count, gen_count), jnp.float32),
            pltpu.VMEM((row_count, stor_count), jnp.float32),
            pltpu.VMEM((8, row_count), jnp.float32),
        ),
        in_specs=[in_vmem] * len(operands),
        out_specs=(in_vmem,) * 4,
        name="update",
        compiler_params=pltpu.CompilerParams(vmem_limit_bytes=VMEM_LIMIT),
    )(*operands)


def gathered_duals(sent):
    own = lax.all_to_all(sent, CHIPS, 0, 0, tiled=True).reshape(-1, sent.shape[2])
    return own, swapped(own)


def doubled(x, axis, size, step, dim):
    other = lax.ppermute(x, axis, [(i, i ^ step) for i in range(size)])
    first = (lax.axis_index(axis) // step) % 2 == 0
    return jnp.where(
        first, jnp.concatenate([x, other], axis=dim), jnp.concatenate([other, x], axis=dim)
    )


def gathered_early(share):
    share_len, row_count = share.shape
    held = share.astype(jnp.bfloat16).reshape(1, 1, 1, share_len, row_count)
    for dim, step in enumerate((4, 2, 1)):
        held = doubled(held, "z", Z, step, dim)
    held = held.reshape(Z, 1, share_len, row_count)
    near = [held]
    for step in (1, 2, 3):
        near.append(lax.ppermute(held, "x", [(i, i ^ step) for i in range(X)]))
    index = lax.axis_index("x")
    low, high = index % 2 == 0, index // 2 == 0

    def pair(first, second):
        return jnp.where(
            low,
            jnp.concatenate([first, second], axis=1),
            jnp.concatenate([second, first], axis=1),
        )

    mine, far = pair(near[0], near[1]), pair(near[2], near[3])
    held = jnp.where(
        high, jnp.concatenate([mine, far], axis=1), jnp.concatenate([far, mine], axis=1)
    )
    own = held.reshape(-1, row_count)
    return own, swapped(own)


def hour_sums(row_count, later):
    row = jnp.arange(row_count, dtype=jnp.int32)
    same = (row[:, None] // HOURS) == (row[None, :] // HOURS)
    side = (row[None, :] >= row[:, None]) if later else (row[None, :] <= row[:, None])
    return jnp.where(same & side, 1.0, 0.0).astype(jnp.float32)


def summed_hours(values, later):
    return jnp.dot(
        hour_sums(values.shape[0], later),
        values,
        precision=lax.Precision.HIGHEST,
        preferred_element_type=jnp.float32,
    )


def dual_step(dual_now, image_term, step_size, low_bound, high_bound):
    shifted = dual_now + step_size * image_term
    return shifted - step_size * jnp.clip(shifted / step_size, low_bound, high_bound)


def shards(
    ptdf,
    load,
    ratings,
    line_index,
    gen_bus,
    gen_quad,
    gen_lin,
    gen_max,
    gen_start,
    stor_bus,
    stor_quad,
    stor_rate,
    stor_energy,
    stor_start,
    lam_start,
    mu_start,
    omega_start,
):
    row_count = load.shape[0]
    line_count, bus_count = ptdf.shape
    gen_count = gen_bus.shape[0]
    stor_count = stor_bus.shape[0]
    area_count = Z * X * CORES
    chip_count = Z * X
    slots = max(8, (gen_count + area_count - 1) // area_count)
    share_len = line_count // area_count
    core = lax.axis_index("core")
    area = (lax.axis_index("z") * X + lax.axis_index("x")) * CORES + core

    target = gen_bus // bus_count
    local_bus = gen_bus % bus_count
    order = jnp.arange(gen_count, dtype=jnp.int32)
    earlier = (target[:, None] == target[None, :]) & (order[None, :] < order[:, None])
    column = target * slots + jnp.sum(earlier.astype(jnp.int32), axis=1)
    slot_of = jnp.arange(area_count * slots, dtype=jnp.int32)
    placed = slot_of[:, None] == column[None, :]
    slot_bus = jnp.sum(jnp.where(placed, local_bus[None, :] + 1, 0), axis=1) - 1
    wanted = lax.all_to_all(slot_bus.reshape(area_count, slots), AREAS, 0, 0, tiled=True)

    dual_flow = mu_start.T
    dual_own, dual_other = gathered_early(dual_flow)

    bus_ids = jnp.arange(bus_count, dtype=jnp.int32)
    sel_gen = (wanted.reshape(-1)[:, None] == bus_ids[None, :]).astype(jnp.bfloat16)
    sel_stor = (stor_bus[:, None] == bus_ids[None, :]).astype(jnp.bfloat16)
    sent_columns = lax.dot_general(
        sel_gen, ptdf, CONTRACT_MINOR, preferred_element_type=jnp.float32
    ).astype(jnp.bfloat16)
    columns = lax.all_to_all(sent_columns, AREAS, 0, 0, tiled=True)
    weight_stor = lax.dot_general(
        ptdf, sel_stor, CONTRACT_MINOR, preferred_element_type=jnp.float32
    ).astype(jnp.bfloat16)

    def by_core(x):
        split = x.reshape(chip_count, CORES, share_len, x.shape[1])
        own = lax.dynamic_index_in_dim(split, core, 1, keepdims=False)
        other = lax.dynamic_index_in_dim(split, 1 - core, 1, keepdims=False)
        return own.reshape(-1, x.shape[1]), other.reshape(-1, x.shape[1])

    weight_own, weight_other, halves = weights_and_prices(
        core,
        columns.reshape(-1, line_count),
        column,
        *by_core(weight_stor),
        dual_own,
        dual_other,
    )
    load_part = lax.dot_general(
        ptdf, load.astype(jnp.bfloat16), CONTRACT_MINOR, preferred_element_type=jnp.float32
    )
    load_own, load_other = by_core(load_part)
    load_flow = load_own + swapped(load_other)
    load_total = jnp.sum(load, axis=1)

    weight_far = swapped(weight_other)
    limit = jnp.take(ratings, lax.dynamic_slice_in_dim(line_index, area * share_len, share_len))[:, None]
    hour_of = jnp.arange(row_count, dtype=jnp.int32) % HOURS
    last_hour = (hour_of == HOURS - 1)[:, None]
    half_energy = (0.5 * stor_energy)[None, :]
    low_bound = jnp.where(last_hour, jnp.zeros_like(half_energy), -half_energy)
    high_bound = jnp.where(last_hour, jnp.zeros_like(half_energy), half_energy)
    total_units = (gen_count + stor_count) * area_count
    gen_now, stor_now = (gen_start, stor_start)
    gen_old, stor_old = (gen_start, stor_start)
    price_level, dual_store = (lam_start, omega_start)
    for iteration in range(2):
        if iteration > 0:
            halves = later_prices(dual_own, dual_other, weight_own, weight_other)
        back = summed_hours(dual_store, True)
        held = bases(
            price_level,
            gen_quad,
            gen_lin,
            stor_quad,
            back,
            gen_now,
            stor_now,
            (gen_old, stor_old) if iteration > 0 else (),
        )
        bar_low, gen_next, stor_next, total = updated(
            summed_pairs(halves), held, gen_max, stor_rate
        )
        balance = total[0] - load_total
        stor_bar = 2.0 * stor_next - stor_now
        flow_part = (
            lax.dot_general(weight_own, bar_low, CONTRACT_MINOR, preferred_element_type=jnp.float32)
            + lax.dot_general(
                weight_far, swapped(bar_low), CONTRACT_MINOR, preferred_element_type=jnp.float32
            )
            - load_flow
        )
        balance = balance + swapped(balance)
        high = rounded(balance)
        lanes = 128
        strips = row_count // lanes
        tail = jnp.concatenate(
            [
                high.reshape(strips, lanes),
                (balance - high).reshape(strips, lanes),
                jnp.zeros((8 - 2 * strips, lanes), jnp.float32),
            ],
            axis=0,
        )
        body = flow_part.reshape(chip_count, share_len, row_count)
        sent = jnp.concatenate(
            [body[:, :, i * lanes : (i + 1) * lanes] for i in range(strips)]
            + [jnp.broadcast_to(tail[None], (chip_count, 8, lanes))],
            axis=1,
        ).astype(jnp.bfloat16)
        received = lax.all_to_all(sent, CHIPS, 0, 0, tiled=True)
        tail, dual_flow, *spread = dual_updated(received, dual_flow, limit, iteration == 0)
        balance = (tail[:strips] + tail[strips : 2 * strips]).reshape(row_count)
        if iteration == 0:
            dual_own, dual_other = gathered_duals(spread[0])
        price_level = price_level + KAPPA / total_units * balance
        dual_store = dual_step(
            dual_store, summed_hours(stor_bar, False), SIGMA_STORE, low_bound, high_bound
        )
        gen_old, stor_old = (gen_now, stor_now)
        gen_now, stor_now = (gen_next, stor_next)
    return (gen_now, stor_now, price_level, dual_flow.T, dual_store)


def solution(mesh):
    fine = Mesh(
        mesh.devices.reshape(mesh.shape["lines"], Z, X, CORES), ("lines", "z", "x", "core")
    )
    by_area = P(AREAS)
    by_column = P(None, AREAS)
    return jax.shard_map(
        shards,
        mesh=fine,
        in_specs=(
            P("lines", AREAS),
            by_column,
            P(),
            P("lines"),
            by_area,
            by_area,
            by_area,
            by_area,
            by_column,
            by_area,
            by_area,
            by_area,
            by_area,
            by_column,
            P(),
            P(None, ("lines", *AREAS)),
            by_column,
        ),
        out_specs=(by_column, by_column, P(), P(None, ("lines", *AREAS)), by_column),
        check_vma=False,
    )
```

```python
import jax
import jax.numpy as jnp
from jax import lax
from jax.experimental import pallas as pl
from jax.experimental.pallas import tpu as pltpu
from jax.sharding import Mesh
from jax.sharding import PartitionSpec as P

HOURS = 24
Z, X, CORES = (8, 4, 2)


TAU = 0.25
SIGMA_FLOW = 4.0
SIGMA_STORE = 0.25
KAPPA = 1.0
THETA = 0.5

VMEM_LIMIT = 16 * 1024 * 1024
AREAS = ("z", "x", "core")
CHIPS = ("z", "x")


def swapped(x):
    return lax.ppermute(x, "core", [(0, 1), (1, 0)])


CONTRACT_MAJOR = (((0,), (0,)), ((), ()))
CONTRACT_MINOR = (((1,), (1,)), ((), ()))


def from_side(x, step):
    return lax.ppermute(x, "lines", [(i, i ^ step) for i in range(4)])


def with_side(x, step):
    other = from_side(x, step)
    return (x.astype(jnp.float32) + other.astype(jnp.float32)).astype(jnp.bfloat16)


def summed_pairs(halves):
    first = with_side(halves[0], 1)
    second = with_side(halves[1], 3)
    return first, from_side(first, 3), second, from_side(second, 1)


def store_price(dual_own, dual_other, weight_own, weight_other, first, second):
    price = lax.dot_general(
        dual_own[...], weight_own[...], CONTRACT_MAJOR, preferred_element_type=jnp.float32
    ) + lax.dot_general(
        dual_other[...], weight_other[...], CONTRACT_MAJOR, preferred_element_type=jnp.float32
    )
    rows = first.shape[0]
    first[...] = price[:rows].astype(jnp.bfloat16)
    second[...] = price[rows:].astype(jnp.bfloat16)


def weights_body(
    core,
    columns,
    column,
    stor_own,
    stor_other,
    dual_own,
    dual_other,
    weight_own,
    weight_other,
    first,
    second,
    split,
):
    slot_count, gen_count = columns.shape[0], column.shape[1]
    slot = lax.broadcasted_iota(jnp.int32, (slot_count, gen_count), 0)
    pick = jnp.where(slot == column[...], 1.0, 0.0).astype(jnp.bfloat16)
    weight = lax.dot_general(
        columns[...], pick, CONTRACT_MAJOR, preferred_element_type=jnp.float32
    )
    split[...] = weight.astype(jnp.bfloat16).reshape(split.shape)
    share_len = split.shape[1]
    mine = core[0]
    for chip in range(split.shape[0] // CORES):
        rows = slice(chip * share_len, (chip + 1) * share_len)
        weight_own[rows, :gen_count] = split[CORES * chip + mine]
        weight_other[rows, :gen_count] = split[CORES * chip + 1 - mine]
    weight_own[:, gen_count:] = stor_own[...]
    weight_other[:, gen_count:] = stor_other[...]
    store_price(dual_own, dual_other, weight_own, weight_other, first, second)


def price_body(dual_own, dual_other, weight_own, weight_other, first, second):
    store_price(dual_own, dual_other, weight_own, weight_other, first, second)


def in_fast(*arrays):
    return tuple(pltpu.with_memory_space_constraint(x, pltpu.VMEM) for x in arrays)


def in_main(*arrays):
    return tuple(pltpu.with_memory_space_constraint(x, pltpu.HBM) for x in arrays)


def half_prices(row_count, units):
    half = pltpu.VMEM((row_count // 2, units), jnp.bfloat16)
    return (half, half)


def weights_and_prices(core, columns, column, stor_own, stor_other, dual_own, dual_other):
    half_lines, row_count = dual_own.shape
    gen_count = column.shape[0]
    units = gen_count + stor_own.shape[1]
    weight = pltpu.HBM((half_lines, units), jnp.bfloat16)
    in_vmem = pl.BlockSpec(memory_space=pltpu.VMEM)
    share_len = columns.shape[1] // (Z * X * CORES)
    own, other, first, second = pl.pallas_call(
        weights_body,
        out_shape=(weight, weight, *half_prices(row_count, units)),
        in_specs=[pl.BlockSpec(memory_space=pltpu.SMEM)] + [in_vmem] * 6,
        out_specs=(in_vmem,) * 4,
        scratch_shapes=[pltpu.VMEM((Z * X * CORES, share_len, gen_count), jnp.bfloat16)],
        name="weights",
        compiler_params=pltpu.CompilerParams(vmem_limit_bytes=VMEM_LIMIT),
    )(
        core.reshape(1),
        *in_fast(columns),
        column.reshape(1, -1),
        *in_main(stor_own, stor_other, dual_own, dual_other),
    )
    return own, other, (first, second)


def later_prices(dual_own, dual_other, weight_own, weight_other):
    in_vmem = pl.BlockSpec(memory_space=pltpu.VMEM)
    return pl.pallas_call(
        price_body,
        out_shape=half_prices(dual_own.shape[1], weight_own.shape[1]),
        in_specs=[in_vmem] * 4,
        out_specs=(in_vmem,) * 2,
        name="prices",
        compiler_params=pltpu.CompilerParams(vmem_limit_bytes=VMEM_LIMIT),
    )(*in_fast(dual_own, dual_other), *in_main(weight_own, weight_other))


def dual_body(received, dual, limit, tail, dual_next, *sent):
    total = jnp.sum(received[...].astype(jnp.float32), axis=0)
    share_len = dual.shape[0]
    strips = dual.shape[1] // total.shape[1]
    flow = jnp.concatenate(
        [total[i * share_len : (i + 1) * share_len] for i in range(strips)], axis=1
    )
    tail[...] = total[strips * share_len :]
    bound = limit[...]
    moved = dual_step(dual[...], flow, SIGMA_FLOW, -bound, bound)
    dual_next[...] = moved
    for out in sent:
        out[...] = jnp.broadcast_to(moved.astype(jnp.bfloat16)[None], out.shape)


def dual_updated(received, dual, limit, spread):
    chips, _, lanes = received.shape
    in_vmem = pl.BlockSpec(memory_space=pltpu.VMEM)
    out_shape = (
        jax.ShapeDtypeStruct((8, lanes), jnp.float32),
        jax.ShapeDtypeStruct(dual.shape, jnp.float32),
    )
    if spread:
        out_shape += (pltpu.HBM((chips, *dual.shape), jnp.bfloat16),)
    return pl.pallas_call(
        dual_body,
        out_shape=out_shape,
        in_specs=[in_vmem] * 3,
        out_specs=(in_vmem,) * len(out_shape),
        name="duals",
        compiler_params=pltpu.CompilerParams(vmem_limit_bytes=VMEM_LIMIT),
    )(*in_fast(received), dual, limit)


def flow_body(bar, bar_far, weight_own, weight_far, load_flow, balance, sent):
    flow = (
        lax.dot_general(
            weight_own[...], bar[...], CONTRACT_MINOR, preferred_element_type=jnp.float32
        )
        + lax.dot_general(
            weight_far[...], bar_far[...], CONTRACT_MINOR, preferred_element_type=jnp.float32
        )
        - load_flow[...]
    )
    chips, rows, lanes = sent.shape
    share_len = flow.shape[0] // chips
    strips = flow.shape[1] // lanes
    for i in range(strips):
        strip = flow[:, i * lanes : (i + 1) * lanes].astype(jnp.bfloat16)
        sent[:, i * share_len : (i + 1) * share_len] = strip.reshape(chips, share_len, lanes)
    level = balance[...]
    high = level.astype(jnp.bfloat16).astype(jnp.float32)
    low = level - high
    tail = [x[:, i * lanes : (i + 1) * lanes] for x in (high, low) for i in range(strips)]
    tail.append(jnp.zeros((rows - strips * share_len - 2 * strips, lanes), jnp.float32))
    tail = jnp.concatenate(tail, axis=0).astype(jnp.bfloat16)
    sent[:, strips * share_len :] = jnp.broadcast_to(tail[None], (chips, *tail.shape))


def flows_to_send(bar, bar_far, weight_own, weight_far, load_flow, balance):
    lanes, chips = 128, Z * X
    rows = load_flow.size // (chips * lanes) + 8
    in_vmem = pl.BlockSpec(memory_space=pltpu.VMEM)
    return pl.pallas_call(
        flow_body,
        out_shape=pltpu.HBM((chips, rows, lanes), jnp.bfloat16),
        in_specs=[in_vmem] * 6,
        out_specs=in_vmem,
        name="flows",
        compiler_params=pltpu.CompilerParams(vmem_limit_bytes=VMEM_LIMIT),
    )(*in_fast(bar, bar_far), *in_main(weight_own, weight_far, load_flow), balance[None, :])


def base_body(level, gen_quad, gen_lin, stor_quad, back, gen_now, stor_now, *refs):
    *old, gen_base, stor_base, gen_held, stor_held = refs
    gen, stor = gen_now[...], stor_now[...]
    gen_mid, stor_mid = gen, stor
    if old:
        gen_mid = gen + THETA * (gen - old[0][...])
        stor_mid = stor + THETA * (stor - old[1][...])
    gen_cost = 2.0 * gen_quad[...] * gen_mid + gen_lin[...] + level[...]
    stor_cost = 2.0 * stor_quad[...] * stor_mid + level[...] + back[...]
    gen_base[...] = gen_mid - TAU * gen_cost
    stor_base[...] = stor_mid - TAU * stor_cost
    gen_held[...] = gen
    stor_held[...] = stor


def update_body(
    first,
    first_far,
    second,
    second_far,
    gen_base,
    stor_base,
    gen_now,
    stor_now,
    gen_max,
    stor_rate,
    bar_low,
    gen_next,
    stor_next,
    total,
):
    row_count, gen_count = gen_now.shape
    half = row_count // 2
    rate = stor_rate[...]
    bars = []
    for i, (near, far) in enumerate(((first, first_far), (second, second_far))):
        rows = slice(i * half, (i + 1) * half)
        change = TAU * (near[...].astype(jnp.float32) + far[...].astype(jnp.float32))
        moved = jnp.clip(gen_base[rows] - change[:, :gen_count], 0.0, gen_max[...])
        shifted = jnp.clip(stor_base[rows] - change[:, gen_count:], -rate, rate)
        gen_next[rows] = moved
        stor_next[rows] = shifted
        bar = jnp.concatenate(
            [2.0 * moved - gen_now[rows], 2.0 * shifted - stor_now[rows]], axis=1
        )
        bar_low[rows] = bar.astype(jnp.bfloat16)
        bars.append(bar)
    total[...] = lax.dot_general(
        jnp.ones((8, bars[0].shape[1]), jnp.float32),
        jnp.concatenate(bars, axis=0),
        CONTRACT_MINOR,
        precision=lax.Precision.HIGHEST,
        preferred_element_type=jnp.float32,
    )


def bases(level, gen_quad, gen_lin, stor_quad, back, gen_now, stor_now, old):
    operands = (
        *in_fast(level[:, None]),
        *in_main(
            gen_quad[None, :],
            gen_lin[None, :],
            stor_quad[None, :],
            back,
            gen_now,
            stor_now,
            *old,
        ),
    )
    in_vmem = pl.BlockSpec(memory_space=pltpu.VMEM)
    gen, stor = pltpu.VMEM(gen_now.shape, jnp.float32), pltpu.VMEM(stor_now.shape, jnp.float32)
    return pl.pallas_call(
        base_body,
        out_shape=(gen, stor, gen, stor),
        in_specs=[in_vmem] * len(operands),
        out_specs=(in_vmem,) * 4,
        name="bases",
        compiler_params=pltpu.CompilerParams(vmem_limit_bytes=VMEM_LIMIT),
    )(*operands)


def updated(pairs, held, gen_max, stor_rate):
    row_count, gen_count = held[0].shape
    stor_count = held[1].shape[1]
    operands = (*in_fast(*pairs, *held), *in_main(gen_max[None, :], stor_rate[None, :]))
    in_vmem = pl.BlockSpec(memory_space=pltpu.VMEM)
    return pl.pallas_call(
        update_body,
        out_shape=(
            pltpu.VMEM((row_count, gen_count + stor_count), jnp.bfloat16),
            pltpu.HBM((row_count, gen_count), jnp.float32),
            pltpu.HBM((row_count, stor_count), jnp.float32),
            pltpu.VMEM((8, row_count), jnp.float32),
        ),
        in_specs=[in_vmem] * len(operands),
        out_specs=(in_vmem,) * 4,
        name="update",
        compiler_params=pltpu.CompilerParams(vmem_limit_bytes=VMEM_LIMIT),
    )(*operands)


def gathered_duals(sent):
    own = lax.all_to_all(sent, CHIPS, 0, 0, tiled=True).reshape(-1, sent.shape[2])
    return own, swapped(own)


def doubled(x, axis, size, step, dim):
    other = lax.ppermute(x, axis, [(i, i ^ step) for i in range(size)])
    first = (lax.axis_index(axis) // step) % 2 == 0
    return jnp.where(
        first, jnp.concatenate([x, other], axis=dim), jnp.concatenate([other, x], axis=dim)
    )


def gathered_early(share):
    share_len, row_count = share.shape
    held = share.astype(jnp.bfloat16).reshape(1, 1, 1, share_len, row_count)
    for dim, step in enumerate((4, 2, 1)):
        held = doubled(held, "z", Z, step, dim)
    held = held.reshape(Z, 1, share_len, row_count)
    near = [held]
    for step in (1, 2, 3):
        near.append(lax.ppermute(held, "x", [(i, i ^ step) for i in range(X)]))
    index = lax.axis_index("x")
    low, high = index % 2 == 0, index // 2 == 0

    def pair(first, second):
        return jnp.where(
            low,
            jnp.concatenate([first, second], axis=1),
            jnp.concatenate([second, first], axis=1),
        )

    mine, far = pair(near[0], near[1]), pair(near[2], near[3])
    held = jnp.where(
        high, jnp.concatenate([mine, far], axis=1), jnp.concatenate([far, mine], axis=1)
    )
    own = held.reshape(-1, row_count)
    return own, swapped(own)


def hour_sums(row_count, later):
    row = jnp.arange(row_count, dtype=jnp.int32)
    same = (row[:, None] // HOURS) == (row[None, :] // HOURS)
    side = (row[None, :] >= row[:, None]) if later else (row[None, :] <= row[:, None])
    return jnp.where(same & side, 1.0, 0.0).astype(jnp.float32)


def summed_hours(values, later):
    return jnp.dot(
        hour_sums(values.shape[0], later),
        values,
        precision=lax.Precision.HIGHEST,
        preferred_element_type=jnp.float32,
    )


def dual_step(dual_now, image_term, step_size, low_bound, high_bound):
    shifted = dual_now + step_size * image_term
    return shifted - step_size * jnp.clip(shifted / step_size, low_bound, high_bound)


def shards(
    ptdf,
    load,
    ratings,
    line_index,
    gen_bus,
    gen_quad,
    gen_lin,
    gen_max,
    gen_start,
    stor_bus,
    stor_quad,
    stor_rate,
    stor_energy,
    stor_start,
    lam_start,
    mu_start,
    omega_start,
):
    row_count = load.shape[0]
    line_count, bus_count = ptdf.shape
    gen_count = gen_bus.shape[0]
    stor_count = stor_bus.shape[0]
    area_count = Z * X * CORES
    chip_count = Z * X
    slots = max(8, (gen_count + area_count - 1) // area_count)
    share_len = line_count // area_count
    core = lax.axis_index("core")
    area = (lax.axis_index("z") * X + lax.axis_index("x")) * CORES + core

    target = gen_bus // bus_count
    local_bus = gen_bus % bus_count
    order = jnp.arange(gen_count, dtype=jnp.int32)
    earlier = (target[:, None] == target[None, :]) & (order[None, :] < order[:, None])
    column = target * slots + jnp.sum(earlier.astype(jnp.int32), axis=1)
    slot_of = jnp.arange(area_count * slots, dtype=jnp.int32)
    placed = slot_of[:, None] == column[None, :]
    slot_bus = jnp.sum(jnp.where(placed, local_bus[None, :] + 1, 0), axis=1) - 1
    wanted = lax.all_to_all(slot_bus.reshape(area_count, slots), AREAS, 0, 0, tiled=True)

    dual_flow = mu_start.T
    dual_own, dual_other = gathered_early(dual_flow)

    bus_ids = jnp.arange(bus_count, dtype=jnp.int32)
    sel_gen = (wanted.reshape(-1)[:, None] == bus_ids[None, :]).astype(jnp.bfloat16)
    sel_stor = (stor_bus[:, None] == bus_ids[None, :]).astype(jnp.bfloat16)
    sent_columns = lax.dot_general(
        sel_gen, ptdf, CONTRACT_MINOR, preferred_element_type=jnp.float32
    ).astype(jnp.bfloat16)
    columns = lax.all_to_all(sent_columns, AREAS, 0, 0, tiled=True)
    weight_stor = lax.dot_general(
        ptdf, sel_stor, CONTRACT_MINOR, preferred_element_type=jnp.float32
    ).astype(jnp.bfloat16)

    def by_core(x):
        split = x.reshape(chip_count, CORES, share_len, x.shape[1])
        own = lax.dynamic_index_in_dim(split, core, 1, keepdims=False)
        other = lax.dynamic_index_in_dim(split, 1 - core, 1, keepdims=False)
        return own.reshape(-1, x.shape[1]), other.reshape(-1, x.shape[1])

    weight_own, weight_other, halves = weights_and_prices(
        core,
        columns.reshape(-1, line_count),
        column,
        *by_core(weight_stor),
        dual_own,
        dual_other,
    )
    load_part = lax.dot_general(
        ptdf, load.astype(jnp.bfloat16), CONTRACT_MINOR, preferred_element_type=jnp.float32
    )
    load_own, load_other = by_core(load_part)
    load_flow = load_own + swapped(load_other)
    load_total = jnp.sum(load, axis=1)

    weight_far = swapped(weight_other)
    limit = jnp.take(ratings, lax.dynamic_slice_in_dim(line_index, area * share_len, share_len))[:, None]
    hour_of = jnp.arange(row_count, dtype=jnp.int32) % HOURS
    last_hour = (hour_of == HOURS - 1)[:, None]
    half_energy = (0.5 * stor_energy)[None, :]
    low_bound = jnp.where(last_hour, jnp.zeros_like(half_energy), -half_energy)
    high_bound = jnp.where(last_hour, jnp.zeros_like(half_energy), half_energy)
    total_units = (gen_count + stor_count) * area_count
    gen_now, stor_now = (gen_start, stor_start)
    gen_old, stor_old = (gen_start, stor_start)
    price_level, dual_store = (lam_start, omega_start)
    for iteration in range(2):
        if iteration > 0:
            halves = later_prices(dual_own, dual_other, weight_own, weight_other)
        back = summed_hours(dual_store, True)
        held = bases(
            price_level,
            gen_quad,
            gen_lin,
            stor_quad,
            back,
            gen_now,
            stor_now,
            (gen_old, stor_old) if iteration > 0 else (),
        )
        bar_low, gen_next, stor_next, total = updated(
            summed_pairs(halves), held, gen_max, stor_rate
        )
        balance = total[0] - load_total
        stor_bar = 2.0 * stor_next - stor_now
        balance = balance + swapped(balance)
        strips = row_count // 128
        sent = flows_to_send(
            bar_low, swapped(bar_low), weight_own, weight_far, load_flow, balance
        )
        received = lax.all_to_all(sent, CHIPS, 0, 0, tiled=True)
        tail, dual_flow, *spread = dual_updated(received, dual_flow, limit, iteration == 0)
        balance = (tail[:strips] + tail[strips : 2 * strips]).reshape(row_count)
        if iteration == 0:
            dual_own, dual_other = gathered_duals(spread[0])
        price_level = price_level + KAPPA / total_units * balance
        dual_store = dual_step(
            dual_store, summed_hours(stor_bar, False), SIGMA_STORE, low_bound, high_bound
        )
        gen_old, stor_old = (gen_now, stor_now)
        gen_now, stor_now = (gen_next, stor_next)
    return (gen_now, stor_now, price_level, dual_flow.T, dual_store)


def solution(mesh):
    fine = Mesh(
        mesh.devices.reshape(mesh.shape["lines"], Z, X, CORES), ("lines", "z", "x", "core")
    )
    by_area = P(AREAS)
    by_column = P(None, AREAS)
    return jax.shard_map(
        shards,
        mesh=fine,
        in_specs=(
            P("lines", AREAS),
            by_column,
            P(),
            P("lines"),
            by_area,
            by_area,
            by_area,
            by_area,
            by_column,
            by_area,
            by_area,
            by_area,
            by_area,
            by_column,
            P(),
            P(None, ("lines", *AREAS)),
            by_column,
        ),
        out_specs=(by_column, by_column, P(), P(None, ("lines", *AREAS)), by_column),
        check_vma=False,
    )
```

```python
import jax
import jax.numpy as jnp
from jax import lax
from jax.experimental import pallas as pl
from jax.experimental.pallas import tpu as pltpu
from jax.sharding import Mesh
from jax.sharding import PartitionSpec as P

HOURS = 24
Z, X, CORES = (8, 4, 2)


TAU = 0.25
SIGMA_FLOW = 4.0
SIGMA_STORE = 0.25
KAPPA = 1.0
THETA = 0.5

VMEM_LIMIT = 16 * 1024 * 1024
AREAS = ("z", "x", "core")
CHIPS = ("z", "x")


def rounded(x):
    return lax.reduce_precision(x, 8, 7)


def swapped(x):
    return lax.ppermute(x, "core", [(0, 1), (1, 0)])


CONTRACT_MAJOR = (((0,), (0,)), ((), ()))
CONTRACT_MINOR = (((1,), (1,)), ((), ()))


def from_side(x, step):
    return lax.ppermute(x, "lines", [(i, i ^ step) for i in range(4)])


def with_side(x, step):
    other = from_side(x, step)
    return (x.astype(jnp.float32) + other.astype(jnp.float32)).astype(jnp.bfloat16)


def summed_pairs(halves):
    first = with_side(halves[0], 1)
    second = with_side(halves[1], 3)
    return first, from_side(first, 3), second, from_side(second, 1)


def store_price(dual_own, dual_other, weight_own, weight_other, first, second):
    price = lax.dot_general(
        dual_own[...], weight_own[...], CONTRACT_MAJOR, preferred_element_type=jnp.float32
    ) + lax.dot_general(
        dual_other[...], weight_other[...], CONTRACT_MAJOR, preferred_element_type=jnp.float32
    )
    rows = first.shape[0]
    first[...] = price[:rows].astype(jnp.bfloat16)
    second[...] = price[rows:].astype(jnp.bfloat16)


def weights_body(
    core,
    columns,
    column,
    stor_own,
    stor_other,
    dual_own,
    dual_other,
    weight_own,
    weight_other,
    first,
    second,
    split,
):
    slot_count, gen_count = columns.shape[0], column.shape[1]
    slot = lax.broadcasted_iota(jnp.int32, (slot_count, gen_count), 0)
    pick = jnp.where(slot == column[...], 1.0, 0.0).astype(jnp.bfloat16)
    weight = lax.dot_general(
        columns[...], pick, CONTRACT_MAJOR, preferred_element_type=jnp.float32
    )
    split[...] = weight.astype(jnp.bfloat16).reshape(split.shape)
    share_len = split.shape[1]
    mine = core[0]
    for chip in range(split.shape[0] // CORES):
        rows = slice(chip * share_len, (chip + 1) * share_len)
        weight_own[rows, :gen_count] = split[CORES * chip + mine]
        weight_other[rows, :gen_count] = split[CORES * chip + 1 - mine]
    weight_own[:, gen_count:] = stor_own[...]
    weight_other[:, gen_count:] = stor_other[...]
    store_price(dual_own, dual_other, weight_own, weight_other, first, second)


def price_body(dual_own, dual_other, weight_own, weight_other, first, second):
    store_price(dual_own, dual_other, weight_own, weight_other, first, second)


def in_fast(*arrays):
    return tuple(pltpu.with_memory_space_constraint(x, pltpu.VMEM) for x in arrays)


def in_main(*arrays):
    return tuple(pltpu.with_memory_space_constraint(x, pltpu.HBM) for x in arrays)


def half_prices(row_count, units):
    half = pltpu.VMEM((row_count // 2, units), jnp.bfloat16)
    return (half, half)


def weights_and_prices(core, columns, column, stor_own, stor_other, dual_own, dual_other):
    half_lines, row_count = dual_own.shape
    gen_count = column.shape[0]
    units = gen_count + stor_own.shape[1]
    weight = pltpu.VMEM((half_lines, units), jnp.bfloat16)
    in_vmem = pl.BlockSpec(memory_space=pltpu.VMEM)
    share_len = columns.shape[1] // (Z * X * CORES)
    own, other, first, second = pl.pallas_call(
        weights_body,
        out_shape=(weight, weight, *half_prices(row_count, units)),
        in_specs=[pl.BlockSpec(memory_space=pltpu.SMEM)] + [in_vmem] * 6,
        out_specs=(in_vmem,) * 4,
        scratch_shapes=[pltpu.VMEM((Z * X * CORES, share_len, gen_count), jnp.bfloat16)],
        name="weights",
        compiler_params=pltpu.CompilerParams(vmem_limit_bytes=VMEM_LIMIT),
    )(
        core.reshape(1),
        *in_fast(columns),
        column.reshape(1, -1),
        *in_main(stor_own, stor_other, dual_own, dual_other),
    )
    return own, other, (first, second)


def later_prices(dual_own, dual_other, weight_own, weight_other):
    in_vmem = pl.BlockSpec(memory_space=pltpu.VMEM)
    return pl.pallas_call(
        price_body,
        out_shape=half_prices(dual_own.shape[1], weight_own.shape[1]),
        in_specs=[in_vmem] * 4,
        out_specs=(in_vmem,) * 2,
        name="prices",
        compiler_params=pltpu.CompilerParams(vmem_limit_bytes=VMEM_LIMIT),
    )(*in_fast(dual_own, dual_other), *in_main(weight_own, weight_other))


def dual_body(received, dual, limit, tail, dual_next, *sent):
    total = jnp.sum(received[...].astype(jnp.float32), axis=0)
    share_len = dual.shape[0]
    strips = dual.shape[1] // total.shape[1]
    flow = jnp.concatenate(
        [total[i * share_len : (i + 1) * share_len] for i in range(strips)], axis=1
    )
    tail[...] = total[strips * share_len :]
    bound = limit[...]
    moved = dual_step(dual[...], flow, SIGMA_FLOW, -bound, bound)
    dual_next[...] = moved
    for out in sent:
        out[...] = jnp.broadcast_to(moved.astype(jnp.bfloat16)[None], out.shape)


def dual_updated(received, dual, limit, spread):
    chips, _, lanes = received.shape
    in_vmem = pl.BlockSpec(memory_space=pltpu.VMEM)
    out_shape = (
        jax.ShapeDtypeStruct((8, lanes), jnp.float32),
        jax.ShapeDtypeStruct(dual.shape, jnp.float32),
    )
    if spread:
        out_shape += (pltpu.HBM((chips, *dual.shape), jnp.bfloat16),)
    return pl.pallas_call(
        dual_body,
        out_shape=out_shape,
        in_specs=[in_vmem] * 3,
        out_specs=(in_vmem,) * len(out_shape),
        name="duals",
        compiler_params=pltpu.CompilerParams(vmem_limit_bytes=VMEM_LIMIT),
    )(*in_fast(received), dual, limit)


def base_body(level, gen_quad, gen_lin, stor_quad, back, gen_now, stor_now, *refs):
    *old, gen_base, stor_base, gen_held, stor_held = refs
    gen, stor = gen_now[...], stor_now[...]
    gen_mid, stor_mid = gen, stor
    if old:
        gen_mid = gen + THETA * (gen - old[0][...])
        stor_mid = stor + THETA * (stor - old[1][...])
    gen_cost = 2.0 * gen_quad[...] * gen_mid + gen_lin[...] + level[...]
    stor_cost = 2.0 * stor_quad[...] * stor_mid + level[...] + back[...]
    gen_base[...] = gen_mid - TAU * gen_cost
    stor_base[...] = stor_mid - TAU * stor_cost
    gen_held[...] = gen
    stor_held[...] = stor


def update_body(
    first,
    first_far,
    second,
    second_far,
    gen_base,
    stor_base,
    gen_now,
    stor_now,
    gen_max,
    stor_rate,
    bar_low,
    gen_next,
    stor_next,
    total,
):
    row_count, gen_count = gen_now.shape
    half = row_count // 2
    rate = stor_rate[...]
    bars = []
    for i, (near, far) in enumerate(((first, first_far), (second, second_far))):
        rows = slice(i * half, (i + 1) * half)
        change = TAU * (near[...].astype(jnp.float32) + far[...].astype(jnp.float32))
        moved = jnp.clip(gen_base[rows] - change[:, :gen_count], 0.0, gen_max[...])
        shifted = jnp.clip(stor_base[rows] - change[:, gen_count:], -rate, rate)
        gen_next[rows] = moved
        stor_next[rows] = shifted
        bar = jnp.concatenate(
            [2.0 * moved - gen_now[rows], 2.0 * shifted - stor_now[rows]], axis=1
        )
        bar_low[rows] = bar.astype(jnp.bfloat16)
        bars.append(bar)
    total[...] = lax.dot_general(
        jnp.ones((8, bars[0].shape[1]), jnp.float32),
        jnp.concatenate(bars, axis=0),
        CONTRACT_MINOR,
        precision=lax.Precision.HIGHEST,
        preferred_element_type=jnp.float32,
    )


def bases(level, gen_quad, gen_lin, stor_quad, back, gen_now, stor_now, old):
    operands = (
        *in_fast(level[:, None]),
        *in_main(
            gen_quad[None, :],
            gen_lin[None, :],
            stor_quad[None, :],
            back,
            gen_now,
            stor_now,
            *old,
        ),
    )
    in_vmem = pl.BlockSpec(memory_space=pltpu.VMEM)
    gen, stor = pltpu.VMEM(gen_now.shape, jnp.float32), pltpu.VMEM(stor_now.shape, jnp.float32)
    return pl.pallas_call(
        base_body,
        out_shape=(gen, stor, gen, stor),
        in_specs=[in_vmem] * len(operands),
        out_specs=(in_vmem,) * 4,
        name="bases",
        compiler_params=pltpu.CompilerParams(vmem_limit_bytes=VMEM_LIMIT),
    )(*operands)


def updated(pairs, held, gen_max, stor_rate, place):
    row_count, gen_count = held[0].shape
    stor_count = held[1].shape[1]
    operands = (*in_fast(*pairs, *held), *in_main(gen_max[None, :], stor_rate[None, :]))
    in_vmem = pl.BlockSpec(memory_space=pltpu.VMEM)
    return pl.pallas_call(
        update_body,
        out_shape=(
            pltpu.VMEM((row_count, gen_count + stor_count), jnp.bfloat16),
            place((row_count, gen_count), jnp.float32),
            place((row_count, stor_count), jnp.float32),
            pltpu.VMEM((8, row_count), jnp.float32),
        ),
        in_specs=[in_vmem] * len(operands),
        out_specs=(in_vmem,) * 4,
        name="update",
        compiler_params=pltpu.CompilerParams(vmem_limit_bytes=VMEM_LIMIT),
    )(*operands)


def gathered_duals(sent):
    own = lax.all_to_all(sent, CHIPS, 0, 0, tiled=True).reshape(-1, sent.shape[2])
    return own, swapped(own)


def doubled(x, axis, size, step, dim):
    other = lax.ppermute(x, axis, [(i, i ^ step) for i in range(size)])
    first = (lax.axis_index(axis) // step) % 2 == 0
    return jnp.where(
        first, jnp.concatenate([x, other], axis=dim), jnp.concatenate([other, x], axis=dim)
    )


def gathered_early(share):
    share_len, row_count = share.shape
    held = share.astype(jnp.bfloat16).reshape(1, 1, 1, share_len, row_count)
    for dim, step in enumerate((4, 2, 1)):
        held = doubled(held, "z", Z, step, dim)
    held = held.reshape(Z, 1, share_len, row_count)
    near = [held]
    for step in (1, 2, 3):
        near.append(lax.ppermute(held, "x", [(i, i ^ step) for i in range(X)]))
    index = lax.axis_index("x")
    low, high = index % 2 == 0, index // 2 == 0

    def pair(first, second):
        return jnp.where(
            low,
            jnp.concatenate([first, second], axis=1),
            jnp.concatenate([second, first], axis=1),
        )

    mine, far = pair(near[0], near[1]), pair(near[2], near[3])
    held = jnp.where(
        high, jnp.concatenate([mine, far], axis=1), jnp.concatenate([far, mine], axis=1)
    )
    own = held.reshape(-1, row_count)
    return own, swapped(own)


def hour_sums(row_count, later):
    row = jnp.arange(row_count, dtype=jnp.int32)
    same = (row[:, None] // HOURS) == (row[None, :] // HOURS)
    side = (row[None, :] >= row[:, None]) if later else (row[None, :] <= row[:, None])
    return jnp.where(same & side, 1.0, 0.0).astype(jnp.float32)


def summed_hours(values, later):
    return jnp.dot(
        hour_sums(values.shape[0], later),
        values,
        precision=lax.Precision.HIGHEST,
        preferred_element_type=jnp.float32,
    )


def dual_step(dual_now, image_term, step_size, low_bound, high_bound):
    shifted = dual_now + step_size * image_term
    return shifted - step_size * jnp.clip(shifted / step_size, low_bound, high_bound)


def shards(
    ptdf,
    load,
    ratings,
    line_index,
    gen_bus,
    gen_quad,
    gen_lin,
    gen_max,
    gen_start,
    stor_bus,
    stor_quad,
    stor_rate,
    stor_energy,
    stor_start,
    lam_start,
    mu_start,
    omega_start,
):
    row_count = load.shape[0]
    line_count, bus_count = ptdf.shape
    gen_count = gen_bus.shape[0]
    stor_count = stor_bus.shape[0]
    area_count = Z * X * CORES
    chip_count = Z * X
    slots = max(8, (gen_count + area_count - 1) // area_count)
    share_len = line_count // area_count
    core = lax.axis_index("core")
    area = (lax.axis_index("z") * X + lax.axis_index("x")) * CORES + core

    target = gen_bus // bus_count
    local_bus = gen_bus % bus_count
    order = jnp.arange(gen_count, dtype=jnp.int32)
    earlier = (target[:, None] == target[None, :]) & (order[None, :] < order[:, None])
    column = target * slots + jnp.sum(earlier.astype(jnp.int32), axis=1)
    slot_of = jnp.arange(area_count * slots, dtype=jnp.int32)
    placed = slot_of[:, None] == column[None, :]
    slot_bus = jnp.sum(jnp.where(placed, local_bus[None, :] + 1, 0), axis=1) - 1
    wanted = lax.all_to_all(slot_bus.reshape(area_count, slots), AREAS, 0, 0, tiled=True)

    dual_flow = mu_start.T
    dual_own, dual_other = gathered_early(dual_flow)

    bus_ids = jnp.arange(bus_count, dtype=jnp.int32)
    sel_gen = (wanted.reshape(-1)[:, None] == bus_ids[None, :]).astype(jnp.bfloat16)
    sel_stor = (stor_bus[:, None] == bus_ids[None, :]).astype(jnp.bfloat16)
    sent_columns = lax.dot_general(
        sel_gen, ptdf, CONTRACT_MINOR, preferred_element_type=jnp.float32
    ).astype(jnp.bfloat16)
    columns = lax.all_to_all(sent_columns, AREAS, 0, 0, tiled=True)
    weight_stor = lax.dot_general(
        ptdf, sel_stor, CONTRACT_MINOR, preferred_element_type=jnp.float32
    ).astype(jnp.bfloat16)

    def by_core(x):
        split = x.reshape(chip_count, CORES, share_len, x.shape[1])
        own = lax.dynamic_index_in_dim(split, core, 1, keepdims=False)
        other = lax.dynamic_index_in_dim(split, 1 - core, 1, keepdims=False)
        return own.reshape(-1, x.shape[1]), other.reshape(-1, x.shape[1])

    weight_own, weight_other, halves = weights_and_prices(
        core,
        columns.reshape(-1, line_count),
        column,
        *by_core(weight_stor),
        dual_own,
        dual_other,
    )
    load_part = lax.dot_general(
        ptdf, load.astype(jnp.bfloat16), CONTRACT_MINOR, preferred_element_type=jnp.float32
    )
    load_own, load_other = by_core(load_part)
    load_flow = load_own + swapped(load_other)
    load_total = jnp.sum(load, axis=1)

    weight_far = swapped(weight_other)
    limit = jnp.take(ratings, lax.dynamic_slice_in_dim(line_index, area * share_len, share_len))[:, None]
    hour_of = jnp.arange(row_count, dtype=jnp.int32) % HOURS
    last_hour = (hour_of == HOURS - 1)[:, None]
    half_energy = (0.5 * stor_energy)[None, :]
    low_bound = jnp.where(last_hour, jnp.zeros_like(half_energy), -half_energy)
    high_bound = jnp.where(last_hour, jnp.zeros_like(half_energy), half_energy)
    total_units = (gen_count + stor_count) * area_count
    gen_now, stor_now = (gen_start, stor_start)
    gen_old, stor_old = (gen_start, stor_start)
    price_level, dual_store = (lam_start, omega_start)
    for iteration in range(2):
        if iteration > 0:
            halves = later_prices(dual_own, dual_other, weight_own, weight_other)
        back = summed_hours(dual_store, True)
        held = bases(
            price_level,
            gen_quad,
            gen_lin,
            stor_quad,
            back,
            gen_now,
            stor_now,
            (gen_old, stor_old) if iteration > 0 else (),
        )
        bar_low, gen_next, stor_next, total = updated(
            summed_pairs(halves),
            held,
            gen_max,
            stor_rate,
            pltpu.VMEM if iteration == 0 else pltpu.HBM,
        )
        balance = total[0] - load_total
        stor_bar = 2.0 * stor_next - stor_now
        flow_part = (
            lax.dot_general(weight_own, bar_low, CONTRACT_MINOR, preferred_element_type=jnp.float32)
            + lax.dot_general(
                weight_far, swapped(bar_low), CONTRACT_MINOR, preferred_element_type=jnp.float32
            )
            - load_flow
        )
        balance = balance + swapped(balance)
        high = rounded(balance)
        lanes = 128
        strips = row_count // lanes
        tail = jnp.concatenate(
            [
                high.reshape(strips, lanes),
                (balance - high).reshape(strips, lanes),
                jnp.zeros((8 - 2 * strips, lanes), jnp.float32),
            ],
            axis=0,
        )
        body = flow_part.reshape(chip_count, share_len, row_count)
        sent = jnp.concatenate(
            [body[:, :, i * lanes : (i + 1) * lanes] for i in range(strips)]
            + [jnp.broadcast_to(tail[None], (chip_count, 8, lanes))],
            axis=1,
        ).astype(jnp.bfloat16)
        received = lax.all_to_all(sent, CHIPS, 0, 0, tiled=True)
        tail, dual_flow, *spread = dual_updated(received, dual_flow, limit, iteration == 0)
        balance = (tail[:strips] + tail[strips : 2 * strips]).reshape(row_count)
        if iteration == 0:
            dual_own, dual_other = gathered_duals(spread[0])
        price_level = price_level + KAPPA / total_units * balance
        dual_store = dual_step(
            dual_store, summed_hours(stor_bar, False), SIGMA_STORE, low_bound, high_bound
        )
        gen_old, stor_old = (gen_now, stor_now)
        gen_now, stor_now = (gen_next, stor_next)
    return (gen_now, stor_now, price_level, dual_flow.T, dual_store)


def solution(mesh):
    fine = Mesh(
        mesh.devices.reshape(mesh.shape["lines"], Z, X, CORES), ("lines", "z", "x", "core")
    )
    by_area = P(AREAS)
    by_column = P(None, AREAS)
    return jax.shard_map(
        shards,
        mesh=fine,
        in_specs=(
            P("lines", AREAS),
            by_column,
            P(),
            P("lines"),
            by_area,
            by_area,
            by_area,
            by_area,
            by_column,
            by_area,
            by_area,
            by_area,
            by_area,
            by_column,
            P(),
            P(None, ("lines", *AREAS)),
            by_column,
        ),
        out_specs=(by_column, by_column, P(), P(None, ("lines", *AREAS)), by_column),
        check_vma=False,
    )
```
